8 devices in a mesh: dp: 2 (over z, y), tp: 4 (over x, core).
Axes of the slice: x: 2, y: 2, z: 1, core: 2. Of those that a mesh axis runs over, the one named last changes fastest.
Arguments:
- hidden: bfloat16 [6, 192, 8192], P('dp', 'tp'), parts along dimension 0
- positions: int32 [6, 192], P('dp', 'tp'), parts along dimension 0
- doc_ids: int32 [6, 192], P('dp', 'tp'), parts along dimension 0
- norm_gain: bfloat16 [8192], replicated
- w_query: bfloat16 [8192, 8192], P(None, 'tp')
- w_key: bfloat16 [8192, 1024], P(None, 'tp')
- w_value: bfloat16 [8192, 1024], P(None, 'tp')
- w_out: bfloat16 [8192, 8192], P('tp')
- grad_out: bfloat16 [6, 192, 8192], P('dp', 'tp'), parts along dimension 0
Outputs:
- output 1: bfloat16 [6, 192, 8192], P('dp', 'tp'), parts along dimension 0
- output 2: bfloat16 [6, 192, 8192], P('dp', 'tp'), parts along dimension 0
- output 3: float32 [16384], P('dp'), parts along dimension 0
- output 4: float32 [16384, 8192], P('dp', 'tp'), parts along dimension 0
- output 5: float32 [16384, 1024], P('dp', 'tp'), parts along dimension 0
- output 6: float32 [16384, 1024], P('dp', 'tp'), parts along dimension 0
- output 7: float32 [16384, 8192], P(('dp', 'tp')), parts along dimension 0
There are 2 independent parts. The reference program is written for one: setup_inputs(seed, part) draws one part's arguments, and reference() takes and returns one part's arrays. A program takes and returns all parts, laid end to end along the dimension named above; an argument that names none is the same for every part.
All inputs are finite; a program needn't handle non-finite values.
Results may differ from the reference program's by a relative error of at most 0.0102642.
Values are sent between devices in bfloat16 or wider.
A program may use at most 1 GiB of HBM per device.

```python
import jax
import jax.numpy as jnp
from jax import lax

BATCH_ROWS = 3
SEQ_LEN = 192
MODEL_DIM = 8192
NUM_HEADS = 64
NUM_KV_HEADS = 8
HEAD_DIM = 128
NORM_EPS = 1e-5
ROPE_BASE = 10000.0


def draw_documents(doc_key):
    doc_mean = max(4, SEQ_LEN // 8)
    token_idx = jnp.arange(SEQ_LEN, dtype=jnp.int32)
    starts = jax.random.randint(doc_key, (BATCH_ROWS, SEQ_LEN), 0, doc_mean) == 0
    starts = starts | (token_idx == 0)[None, :]
    doc_ids = jnp.cumsum(starts.astype(jnp.int32), axis=1) - 1
    begins = lax.cummax(jnp.where(starts, token_idx[None, :], 0), axis=1)
    return (token_idx[None, :] - begins).astype(jnp.int32), doc_ids.astype(jnp.int32)


def setup_inputs(seed: int = 0, part: int = 0) -> dict:
    part_key = jax.random.fold_in(jax.random.key(seed), part)
    shared_key = jax.random.key(seed + 1)
    k_hidden, k_grad, k_doc = jax.random.split(part_key, 3)
    k_gain, k_query, k_key, k_value, k_out = jax.random.split(shared_key, 5)
    positions, doc_ids = draw_documents(k_doc)
    in_scale = MODEL_DIM ** -0.5
    out_scale = 2.0 * (NUM_HEADS * HEAD_DIM) ** -0.5
    q_width = NUM_HEADS * HEAD_DIM
    kv_width = NUM_KV_HEADS * HEAD_DIM
    return {
        'hidden': jax.random.normal(k_hidden, (BATCH_ROWS, SEQ_LEN, MODEL_DIM), jnp.float32).astype(jnp.bfloat16),
        'positions': positions,
        'doc_ids': doc_ids,
        'norm_gain': (1.0 + 0.3 * jax.random.normal(k_gain, (MODEL_DIM,), jnp.float32)).astype(jnp.bfloat16),
        'w_query': (in_scale * jax.random.normal(k_query, (MODEL_DIM, q_width), jnp.float32)).astype(jnp.bfloat16),
        'w_key': (in_scale * jax.random.normal(k_key, (MODEL_DIM, kv_width), jnp.float32)).astype(jnp.bfloat16),
        'w_value': (in_scale * jax.random.normal(k_value, (MODEL_DIM, kv_width), jnp.float32)).astype(jnp.bfloat16),
        'w_out': (out_scale * jax.random.normal(k_out, (q_width, MODEL_DIM), jnp.float32)).astype(jnp.bfloat16),
        'grad_out': jax.random.normal(k_grad, (BATCH_ROWS, SEQ_LEN, MODEL_DIM), jnp.float32).astype(jnp.bfloat16),
    }


def snap_bf16(values):
    return values + lax.stop_gradient(values.astype(jnp.bfloat16).astype(values.dtype) - values)


def rotate_pairs(values, cos_tab, sin_tab):
    pair_view = values.reshape(values.shape[:-1] + (HEAD_DIM // 2, 2))
    even_part = pair_view[..., 0]
    odd_part = pair_view[..., 1]
    turned = jnp.stack([even_part * cos_tab - odd_part * sin_tab, even_part * sin_tab + odd_part * cos_tab], axis=-1)
    return turned.reshape(values.shape)


def reference(hidden, positions, doc_ids, norm_gain, w_query, w_key, w_value, w_out, grad_out):
    group_size = NUM_HEADS // NUM_KV_HEADS
    attn_scale = HEAD_DIM ** -0.5
    inv_freq = ROPE_BASE ** (-jnp.arange(0, HEAD_DIM, 2, dtype=jnp.float32) / HEAD_DIM)
    angles = positions.astype(jnp.float32)[:, :, None] * inv_freq
    cos_tab = jnp.cos(angles)[:, :, None, :]
    sin_tab = jnp.sin(angles)[:, :, None, :]
    token_idx = jnp.arange(SEQ_LEN, dtype=jnp.int32)
    allowed = (doc_ids[:, :, None] == doc_ids[:, None, :]) & (token_idx[None, :] <= token_idx[:, None])[None]

    def head_group(operands):
        query_grp, key_grp, value_grp = operands
        scores = jnp.einsum('bqgd,bkd->bgqk', query_grp, key_grp) * attn_scale
        scores = jnp.where(allowed[:, None], scores, -1e30)
        attn_probs = snap_bf16(jax.nn.softmax(scores, axis=-1))
        return snap_bf16(jnp.einsum('bgqk,bkd->bqgd', attn_probs, value_grp))

    def forward(hidden_f32, gain_f32, wq_f32, wk_f32, wv_f32, wo_f32):
        mean_sq = jnp.mean(hidden_f32 * hidden_f32, axis=-1, keepdims=True)
        normed = snap_bf16(hidden_f32 * lax.rsqrt(mean_sq + NORM_EPS) * gain_f32)
        query_raw = jnp.dot(normed, wq_f32).reshape(BATCH_ROWS, SEQ_LEN, NUM_HEADS, HEAD_DIM)
        key_raw = jnp.dot(normed, wk_f32).reshape(BATCH_ROWS, SEQ_LEN, NUM_KV_HEADS, HEAD_DIM)
        query_rot = snap_bf16(rotate_pairs(query_raw, cos_tab, sin_tab))
        key_rot = snap_bf16(rotate_pairs(key_raw, cos_tab, sin_tab))
        value_rows = snap_bf16(jnp.dot(normed, wv_f32)).reshape(BATCH_ROWS, SEQ_LEN, NUM_KV_HEADS, HEAD_DIM)
        query_groups = jnp.moveaxis(query_rot.reshape(BATCH_ROWS, SEQ_LEN, NUM_KV_HEADS, group_size, HEAD_DIM), 2, 0)
        heads_out = lax.map(jax.checkpoint(head_group), (query_groups, jnp.moveaxis(key_rot, 2, 0), jnp.moveaxis(value_rows, 2, 0)))
        heads_flat = jnp.moveaxis(heads_out, 0, 2).reshape(BATCH_ROWS, SEQ_LEN, NUM_HEADS * HEAD_DIM)
        attn_sum = snap_bf16(jnp.dot(heads_flat, wo_f32))
        return snap_bf16(hidden_f32 + attn_sum)

    attn_out, pullback = jax.vjp(forward, hidden.astype(jnp.float32), norm_gain.astype(jnp.float32), w_query.astype(jnp.float32), w_key.astype(jnp.float32), w_value.astype(jnp.float32), w_out.astype(jnp.float32))
    grad_list = pullback(grad_out.astype(jnp.float32))
    return (attn_out.astype(jnp.bfloat16), grad_list[0].astype(jnp.bfloat16), grad_list[1], grad_list[2], grad_list[3], grad_list[4], grad_list[5])
```

```python
import functools

import jax
import jax.numpy as jnp
from jax import lax
from jax.experimental import pallas as pl
from jax.experimental.pallas import tpu as pltpu
from jax.sharding import PartitionSpec as P


HEAD_DIM = 128
NORM_EPS = 1e-5
ROPE_BASE = 10000.0
BF16 = jnp.bfloat16
F32 = jnp.float32
ANY = pl.BlockSpec(memory_space=pl.ANY)
NN = (((1,), (0,)), ((), ()))
NT = (((1,), (1,)), ((), ()))
TN = (((0,), (0,)), ((), ()))


def dot(a, b, dims=NN):
    return lax.dot_general(a, b, dims, preferred_element_type=F32)


def const_spec(shape):
    return pl.BlockSpec(shape, lambda *_: (0,) * len(shape), pipeline_mode=pl.Buffered(1))


def params(mib, *semantics):
    return pltpu.CompilerParams(dimension_semantics=semantics or ("arbitrary",), vmem_limit_bytes=mib << 20)


def cost(flops, moved):
    return pl.CostEstimate(flops=int(flops), bytes_accessed=int(moved), transcendentals=0)


def swap_pairs(x):
    lane = lax.broadcasted_iota(jnp.int32, x.shape, x.ndim - 1)
    return jnp.where(lane % 2 == 0, pltpu.roll(x, x.shape[-1] - 1, x.ndim - 1), pltpu.roll(x, 1, x.ndim - 1))


def qkv_kernel(q_steps, ha, hb, gain, cos, sin, wq, wk, wv, n_out, inv_out, q_out, k_out, v_out, hs, ks, vs, sem):
    step = pl.program_id(0)
    half = ha.shape[0]

    @pl.when(step == 0)
    def _():
        loads = [pltpu.make_async_copy(ha, hs.at[pl.ds(0, half)], sem.at[0]),
                 pltpu.make_async_copy(hb, hs.at[pl.ds(half, half)], sem.at[1])]
        for c in loads:
            c.start()
        pltpu.make_async_copy(wk, ks, sem.at[2]).start()
        pltpu.make_async_copy(wv, vs, sem.at[3]).start()
        for c in loads:
            c.wait()

        def rows(i, _):
            at = pl.ds(pl.multiple_of(i * 16, 16), 16)
            x = hs[at, :].astype(F32)
            inv = lax.rsqrt(jnp.mean(x * x, axis=-1, keepdims=True) + NORM_EPS)
            n_out[at, :] = (x * inv * gain[...].astype(F32)).astype(BF16)
            inv_out[at, :] = jnp.broadcast_to(inv, (16, 128))
            return 0

        lax.fori_loop(0, 2 * half // 16, rows, 0)

    def rotated(raw):
        parts = []
        for j in range(raw.shape[1] // HEAD_DIM):
            x = raw[:, j * HEAD_DIM:(j + 1) * HEAD_DIM]
            parts.append((x * cos[...] + swap_pairs(x) * sin[...]).astype(BF16))
        return jnp.concatenate(parts, axis=1)

    @pl.when(step < q_steps)
    def _():
        q_out[...] = rotated(dot(n_out[...], wq[...]))

    @pl.when(step == q_steps)
    def _():
        pltpu.make_async_copy(wk, ks, sem.at[2]).wait()
        k_out[...] = rotated(dot(n_out[...], ks[...]))

    @pl.when(step == q_steps + 1)
    def _():
        pltpu.make_async_copy(wv, vs, sem.at[3]).wait()
        v_out[...] = dot(n_out[...], vs[...]).astype(BF16)


def qkv(ha, hb, gain, cos, sin, wq, wk, wv):
    half, width = ha.shape
    tok = 2 * half
    nq, nk = wq.shape[1], wk.shape[1]
    blk = 256
    q_steps = nq // blk
    return pl.pallas_call(
        functools.partial(qkv_kernel, q_steps), name="qkv", grid=(q_steps + 2,),
        in_specs=[ANY, ANY, const_spec((1, width)), const_spec((tok, HEAD_DIM)), const_spec((tok, HEAD_DIM)),
                  pl.BlockSpec((width, blk), lambda i: (0, jnp.minimum(i, q_steps - 1))), ANY, ANY],
        out_specs=[const_spec((tok, width)), const_spec((tok, 128)),
                   pl.BlockSpec((tok, blk), lambda i: (0, jnp.minimum(i, q_steps - 1))),
                   const_spec((tok, nk)), const_spec((tok, nk))],
        out_shape=[jax.ShapeDtypeStruct((tok, width), BF16), jax.ShapeDtypeStruct((tok, 128), F32),
                   jax.ShapeDtypeStruct((tok, nq), BF16), jax.ShapeDtypeStruct((tok, nk), BF16),
                   jax.ShapeDtypeStruct((tok, nk), BF16)],
        scratch_shapes=[pltpu.VMEM((tok, width), BF16), pltpu.VMEM((width, nk), BF16), pltpu.VMEM((width, nk), BF16),
                        pltpu.SemaphoreType.DMA((4,))],
        compiler_params=params(60), cost_estimate=cost(2 * tok * width * (nq + 2 * nk), 2 * width * (nq + 2 * nk)),
    )(ha, hb, gain, cos, sin, wq, wk, wv)


def heads_grad_kernel(ga, gb, w, out, gs, sem):
    half = ga.shape[0]

    @pl.when(pl.program_id(0) == 0)
    def _():
        loads = [pltpu.make_async_copy(ga, gs.at[pl.ds(0, half)], sem.at[0]),
                 pltpu.make_async_copy(gb, gs.at[pl.ds(half, half)], sem.at[1])]
        for c in loads:
            c.start()
        for c in loads:
            c.wait()

    out[...] = dot(gs[...], w[...], NT).astype(BF16)


def heads_grad(ga, gb, w_out):
    half, width = ga.shape
    tok = 2 * half
    n = w_out.shape[0]
    blk = 256
    return pl.pallas_call(
        heads_grad_kernel, name="heads_grad", grid=(n // blk,),
        in_specs=[ANY, ANY, pl.BlockSpec((blk, width), lambda i: (i, 0))],
        out_specs=pl.BlockSpec((tok, blk), lambda i: (0, i)),
        out_shape=jax.ShapeDtypeStruct((tok, n), BF16),
        scratch_shapes=[pltpu.VMEM((tok, width), BF16), pltpu.SemaphoreType.DMA((2,))],
        compiler_params=params(60), cost_estimate=cost(2 * tok * width * n, 2 * width * n),
    )(ga, gb, w_out)


def by_head(a_ref, b_ref, group):
    def flat(r):
        v = r[...]
        return v.reshape(v.shape[0] * v.shape[2], v.shape[3])

    full = jnp.concatenate([flat(a_ref), flat(b_ref)], axis=0)
    return jnp.concatenate([full[:, h * HEAD_DIM:(h + 1) * HEAD_DIM] for h in range(group)], axis=0)


def put(ref, value):
    ref[...] = value.reshape(ref.shape)


def attend_kernel(group, qa, qb, ka, kb, va, vb, mask, oa, ob):
    q = by_head(qa, qb, group)
    k = by_head(ka, kb, 1)
    v = by_head(va, vb, 1)
    seq = k.shape[0]
    scores = dot(q, k, NT) * (HEAD_DIM ** -0.5)
    scores = jnp.where((mask[...] > 0), scores.reshape(group, seq, seq), -1e30).reshape(group * seq, seq)
    top = jnp.max(scores, axis=-1, keepdims=True)
    e = jnp.exp(scores - top)
    probs = (e / jnp.sum(e, axis=-1, keepdims=True)).astype(BF16)
    o = dot(probs, v).astype(BF16)
    o = jnp.concatenate([o[h * seq:(h + 1) * seq] for h in range(group)], axis=1)
    put(oa, o[:seq // 2])
    put(ob, o[seq // 2:])


def head_specs(slots, rows, wide):
    return pl.BlockSpec((slots, 1, rows, wide), lambda r, h: (0, r, 0, h))


def attend(qa, qb, ka, kb, va, vb, mask):
    slots, batch, rows, nq = qa.shape
    kv = ka.shape[3] // HEAD_DIM
    group = nq // ka.shape[3]
    seq = 2 * slots * rows
    qs, ks = head_specs(slots, rows, group * HEAD_DIM), head_specs(slots, rows, HEAD_DIM)
    return pl.pallas_call(
        functools.partial(attend_kernel, group), name="attend", grid=(batch, kv),
        in_specs=[qs, qs, ks, ks, ks, ks, pl.BlockSpec((1, seq, seq), lambda r, h: (r, 0, 0))],
        out_specs=[qs, qs], out_shape=[jax.ShapeDtypeStruct(qa.shape, BF16)] * 2,
        compiler_params=params(60, "arbitrary", "arbitrary"),
        cost_estimate=cost(batch * kv * group * seq * seq * HEAD_DIM * 40, 4 * qa.size * 2),
    )(qa, qb, ka, kb, va, vb, mask)


def attend_back_kernel(group, qa, qb, ka, kb, va, vb, ga, gb, mask, ca, cb, sa, sb, dqa, dqb, dka, dkb, dva, dvb):
    q = by_head(qa, qb, group)
    g = by_head(ga, gb, group)
    k = by_head(ka, kb, 1)
    v = by_head(va, vb, 1)
    cos, sin = by_head(ca, cb, 1), by_head(sa, sb, 1)
    seq = k.shape[0]
    scale = HEAD_DIM ** -0.5
    scores = jnp.where(mask[0] > 0, dot(k, q, NT) * scale, -1e30)
    e = jnp.exp(scores - jnp.max(scores, axis=0, keepdims=True))
    probs = e / jnp.sum(e, axis=0, keepdims=True)
    gp = dot(v, g, NT)
    dots = jnp.sum(probs * gp, axis=0, keepdims=True)
    ds = (probs * (gp - dots) * scale).astype(BF16)
    dv = dot(probs.astype(BF16), g).astype(BF16)
    dk = dot(ds, q)
    dq = dot(ds, k, TN)

    def unrotated(x):
        return (x * cos - swap_pairs(x) * sin).astype(BF16)

    dq = jnp.concatenate([unrotated(dq[h * seq:(h + 1) * seq]) for h in range(group)], axis=1)
    dk = unrotated(dk)
    for lo, hi, value in ((dqa, dqb, dq), (dka, dkb, dk), (dva, dvb, dv)):
        put(lo, value[:seq // 2])
        put(hi, value[seq // 2:])


def attend_back(qa, qb, ka, kb, va, vb, ga, gb, mask, ca, cb, sa, sb):
    slots, batch, rows, nq = qa.shape
    kv = ka.shape[3] // HEAD_DIM
    group = nq // ka.shape[3]
    seq = 2 * slots * rows
    qs, ks = head_specs(slots, rows, group * HEAD_DIM), head_specs(slots, rows, HEAD_DIM)
    ts = pl.BlockSpec((slots, 1, rows, HEAD_DIM), lambda r, h: (0, r, 0, 0))
    return pl.pallas_call(
        functools.partial(attend_back_kernel, group), name="attend_back", grid=(batch, kv),
        in_specs=[qs, qs, ks, ks, ks, ks, qs, qs, pl.BlockSpec((1, seq, group * seq), lambda r, h: (r, 0, 0)), ts, ts, ts, ts],
        out_specs=[qs, qs, ks, ks, ks, ks],
        out_shape=[jax.ShapeDtypeStruct(x.shape, BF16) for x in (qa, qb, ka, kb, va, vb)],
        compiler_params=params(60, "arbitrary", "arbitrary"),
        cost_estimate=cost(batch * kv * group * seq * seq * HEAD_DIM * 60, 8 * qa.size * 2),
    )(qa, qb, ka, kb, va, vb, ga, gb, mask, ca, cb, sa, sb)


def out_share_kernel(o, w, first, second):
    r = dot(o[...], w[...])
    half = first.shape[0]
    first[...] = r[:half].astype(first.dtype)
    second[...] = r[half:].astype(second.dtype)


def out_share(o, w_out, types):
    tok, n = o.shape
    width = w_out.shape[1]
    blk = 1024
    spec = pl.BlockSpec((tok // 2, blk), lambda i: (0, i))
    return pl.pallas_call(
        out_share_kernel, name="out_share", grid=(width // blk,),
        in_specs=[const_spec((tok, n)), pl.BlockSpec((n, blk), lambda i: (0, i))],
        out_specs=[spec, spec], out_shape=[jax.ShapeDtypeStruct((tok // 2, width), t) for t in types],
        compiler_params=params(60), cost_estimate=cost(2 * tok * width * n, 2 * width * n),
    )(o, w_out)


def norm_share_kernel(dq, dk, dv, wq, wk, wv, ha, hb, inv, first, second, gain):
    r = dot(dq[...], wq[...], NT) + dot(dk[...], wk[...], NT) + dot(dv[...], wv[...], NT)
    half = first.shape[0]
    first[...] = r[:half].astype(first.dtype)
    second[...] = r[half:].astype(second.dtype)
    scaled = jnp.concatenate([ha[...], hb[...]], axis=0).astype(F32) * inv[:, :1]
    gain[...] = jnp.sum(r * scaled, axis=0, keepdims=True)


def norm_share(dq, dk, dv, wq, wk, wv, ha, hb, inv, types):
    tok, nq = dq.shape
    nk = dk.shape[1]
    width = wq.shape[0]
    blk = 512
    spec = pl.BlockSpec((tok // 2, blk), lambda i: (0, i))
    return pl.pallas_call(
        norm_share_kernel, name="norm_share", grid=(width // blk,),
        in_specs=[const_spec((tok, nq)), const_spec((tok, nk)), const_spec((tok, nk)),
                  pl.BlockSpec((blk, nq), lambda i: (i, 0)), pl.BlockSpec((blk, nk), lambda i: (i, 0)),
                  pl.BlockSpec((blk, nk), lambda i: (i, 0)), spec, spec, const_spec((tok, 128))],
        out_specs=[spec, spec, pl.BlockSpec((1, blk), lambda i: (0, i))],
        out_shape=[jax.ShapeDtypeStruct((tok // 2, width), t) for t in types] + [jax.ShapeDtypeStruct((1, width), F32)],
        compiler_params=params(60), cost_estimate=cost(2 * tok * width * (nq + 2 * nk), 2 * width * (nq + 2 * nk)),
    )(dq, dk, dv, wq, wk, wv, ha, hb, inv)


def grad_out_kernel(oa, ob, g0, g1, g2, g3, out, ot):
    @pl.when(pl.program_id(0) == 0)
    def _():
        n = oa.shape[1]
        for c in range(0, n, 256):
            ot[c:c + 256, :] = jnp.concatenate([oa[:, c:c + 256], ob[:, c:c + 256]], axis=0).T

    g = jnp.concatenate([g0[...], g1[...], g2[...], g3[...]], axis=0)
    out[...] = dot(ot[...], g)


def grad_w_out(oa, ob, g):
    tok, n = oa.shape
    width = g[0].shape[1]
    blk = 512
    return pl.pallas_call(
        grad_out_kernel, name="grad_w_out", grid=(width // blk,),
        in_specs=[const_spec((tok, n))] * 2 + [pl.BlockSpec((tok // 2, blk), lambda i: (0, i))] * 4,
        out_specs=pl.BlockSpec((n, blk), lambda i: (0, i)), out_shape=jax.ShapeDtypeStruct((n, width), F32),
        scratch_shapes=[pltpu.VMEM((n, 2 * tok), BF16)],
        compiler_params=params(60), cost_estimate=cost(4 * tok * width * n, 4 * width * n),
    )(oa, ob, *g)


def grad_qkv_kernel(na, nb, dqa, dqb, dka, dkb, dva, dvb, gq, gk, gv):
    nt = jnp.concatenate([na[...], nb[...]], axis=0).T
    for lo, hi, out in ((dqa, dqb, gq), (dka, dkb, gk), (dva, dvb, gv)):
        out[...] = dot(nt, jnp.concatenate([lo[...], hi[...]], axis=0))


def grad_w_qkv(na, nb, dqa, dqb, dka, dkb, dva, dvb):
    tok, width = na.shape
    nq, nk = dqa.shape[1], dka.shape[1]
    blk = 512
    return pl.pallas_call(
        grad_qkv_kernel, name="grad_w_qkv", grid=(width // blk,),
        in_specs=[pl.BlockSpec((tok, blk), lambda i: (0, i))] * 2 + [const_spec((tok, nq))] * 2 + [const_spec((tok, nk))] * 4,
        out_specs=[pl.BlockSpec((blk, n), lambda i: (i, 0)) for n in (nq, nk, nk)],
        out_shape=[jax.ShapeDtypeStruct((width, n), F32) for n in (nq, nk, nk)],
        compiler_params=params(60), cost_estimate=cost(4 * tok * width * (nq + 2 * nk), 4 * width * (nq + 2 * nk)),
    )(na, nb, dqa, dqb, dka, dkb, dva, dvb)


def norm_back_kernel(p0, p1, p2, h, g, gain, inv, out):
    dn = p0[...].astype(F32) + p1[...].astype(F32) + p2[...].astype(F32)
    hf = h[...].astype(F32)
    s = inv[:, :1]
    dg = dn * gain[...].astype(F32)
    mean = jnp.mean(dg * hf, axis=-1, keepdims=True)
    out[...] = (g[...].astype(F32) + (s * dg - hf * (s * s * s) * mean)).astype(BF16)


def norm_back(p0, p1, p2, h, g, gain, inv):
    tok, width = h.shape
    blk = 16
    spec = pl.BlockSpec((blk, width), lambda i: (i, 0))
    return pl.pallas_call(
        norm_back_kernel, name="norm_back", grid=(tok // blk,),
        in_specs=[spec] * 5 + [const_spec((1, width)), pl.BlockSpec((blk, 128), lambda i: (i, 0))],
        out_specs=spec, out_shape=jax.ShapeDtypeStruct((tok, width), BF16),
        compiler_params=params(60), cost_estimate=cost(20 * tok * width, 12 * tok * width),
    )(p0, p1, p2, h, g, gain, inv)


def solution(mesh):
    tp_size = mesh.shape['tp']
    beside = [(i, i ^ 1) for i in range(tp_size)]
    across = [(i, i ^ 2) for i in range(tp_size)]
    diagonal = [(i, i ^ 3) for i in range(tp_size)]

    def send(x, pairs):
        return lax.ppermute(x, 'tp', pairs)

    def after(x, *others):
        return lax.optimization_barrier((x,) + others)[0]

    def step(hidden, positions, doc_ids, norm_gain, w_query, w_key, w_value, w_out, grad_out):
        batch, rows, width = hidden.shape
        tok = batch * rows
        nq, nk = w_query.shape[1], w_key.shape[1]
        group = nq // nk
        gain = norm_gain.reshape(1, width)

        ints = jnp.stack([positions, doc_ids])
        ints = jnp.stack([ints, send(ints, beside), send(ints, across), send(ints, diagonal)])
        h0 = hidden.reshape(tok, width)
        g0 = grad_out.reshape(tok, width)
        h2 = send(after(h0, ints), across)
        h1 = send(after(h0, ints), beside)
        g1 = send(after(g0, h1), beside)
        g2 = send(after(g0, h1), across)
        h3 = send(h2, beside)

        pos, doc = ints[:, 0], ints[:, 1]
        lane = jnp.arange(HEAD_DIM)
        inv_freq = ROPE_BASE ** (-(lane // 2 * 2).astype(F32) / HEAD_DIM)
        angles = pos.astype(F32)[..., None] * inv_freq
        cos, sin = jnp.cos(angles), jnp.sin(angles) * jnp.where(lane % 2 == 0, -1.0, 1.0)
        pos_r = jnp.swapaxes(pos, 0, 1).reshape(batch, 4 * rows)
        doc_r = jnp.swapaxes(doc, 0, 1).reshape(batch, 4 * rows)
        allowed = ((doc_r[:, :, None] == doc_r[:, None, :]) & (pos_r[:, None, :] <= pos_r[:, :, None])).astype(F32)
        allowed_t = jnp.tile(jnp.swapaxes(allowed, 1, 2), (1, 1, group)).astype(BF16)

        def heads(x):
            return x.reshape(2, batch, rows, x.shape[1])

        def flat(x):
            return x.reshape(2 * tok, x.shape[3])

        ca, cb, sa, sb = cos[:2], cos[2:], sin[:2], sin[2:]
        na, inv_a, qa, ka, va = qkv(h0, h1, gain, ca.reshape(2 * tok, HEAD_DIM), sa.reshape(2 * tok, HEAD_DIM), w_query, w_key, w_value)
        dha = heads_grad(after(g0, ka), g1, w_out)
        nb, inv_b, qb, kb, vb = qkv(after(h2, dha), h3, gain, cb.reshape(2 * tok, HEAD_DIM), sb.reshape(2 * tok, HEAD_DIM), w_query, w_key, w_value)
        saved = [heads(x) for x in (qa, qb, ka, kb, va, vb)]
        oa, ob = [flat(x) for x in attend(*saved, allowed)]

        p2, p3 = out_share(ob, w_out, (F32, F32))
        p3 = send(p3, beside)
        p0, p1 = out_share(after(oa, p2), w_out, (F32, BF16))
        s2 = (p2 + after(p3, p0)).astype(BF16)
        p1, s2, g2 = lax.optimization_barrier((p1, s2, g2))
        p1 = send(p1, beside)
        s2 = send(s2, across)
        g3 = send(g2, beside)

        dhb = heads_grad(g2, g3, w_out)
        grads = attend_back(*saved, heads(dha), heads(dhb), allowed_t, ca, cb, sa, sb)
        dqa, dqb, dka, dkb, dva, dvb = [flat(x) for x in grads]
        d2, d3, gain_b = norm_share(dqb, dkb, dvb, w_query, w_key, w_value, h2, h3, inv_b, (F32, BF16))
        d3 = send(d3, beside)
        d0, d1, gain_a = norm_share(after(dqa, d2), dka, dva, w_query, w_key, w_value, h0, h1, inv_a, (F32, BF16))
        t2 = (d2 + after(d3, d0).astype(F32)).astype(BF16)
        d1, t2, gg, p1, s2 = lax.optimization_barrier((d1, t2, gain_a + gain_b, p1, s2))
        t2 = send(t2, across)
        d1 = send(d1, beside)
        gg = gg + send(gg, beside)
        attn_rows = (p0 + p1.astype(F32) + s2.astype(F32)).astype(BF16)
        attn_out = (h0 + attn_rows).reshape(hidden.shape)

        g_out = grad_w_out(after(oa, attn_out), ob, (g0, g1, g2, g3))
        gq, gk, gv = grad_w_qkv(after(na, g_out), nb, dqa, dqb, dka, dkb, dva, dvb)
        gg = gg + send(gg, across)
        grad_gain = gg.reshape(width)
        grad_hidden = norm_back(after(d0, gk), d1, t2, h0, g0, gain, inv_a[:tok]).reshape(hidden.shape)
        return (attn_out, grad_hidden, grad_gain, gq, gk, gv, g_out)

    row_spec = P('dp', 'tp', None)
    tok_spec = P('dp', 'tp')
    col_spec = P(None, 'tp')

    return jax.shard_map(
        step, mesh=mesh,
        in_specs=(row_spec, tok_spec, tok_spec, P(), col_spec, col_spec, col_spec, P('tp', None), row_spec),
        out_specs=(row_spec, row_spec, P('dp'), P('dp', 'tp'), P('dp', 'tp'), P('dp', 'tp'), P(('dp', 'tp'), None)),
        check_vma=False)
```

```python
import functools

import jax
import jax.numpy as jnp
from jax import lax
from jax.experimental import pallas as pl
from jax.experimental.pallas import tpu as pltpu
from jax.sharding import PartitionSpec as P


HEAD_DIM = 128
NORM_EPS = 1e-5
ROPE_BASE = 10000.0
LOG2_E = 1.4426950408889634
BF16 = jnp.bfloat16
F32 = jnp.float32
ANY = pl.BlockSpec(memory_space=pl.ANY)
NN = (((1,), (0,)), ((), ()))
NT = (((1,), (1,)), ((), ()))
TN = (((0,), (0,)), ((), ()))


def dot(a, b, dims=NN):
    return lax.dot_general(a, b, dims, preferred_element_type=F32)


def const_spec(shape):
    return pl.BlockSpec(shape, lambda *_: (0,) * len(shape), pipeline_mode=pl.Buffered(1))


def params(mib, *semantics):
    return pltpu.CompilerParams(dimension_semantics=semantics or ("arbitrary",), vmem_limit_bytes=mib << 20)


def cost(flops, moved):
    return pl.CostEstimate(flops=int(flops), bytes_accessed=int(moved), transcendentals=0)


def swap_pairs(x):
    lane = lax.broadcasted_iota(jnp.int32, x.shape, x.ndim - 1)
    return jnp.where(lane % 2 == 0, pltpu.roll(x, x.shape[-1] - 1, x.ndim - 1), pltpu.roll(x, 1, x.ndim - 1))


def qkv_kernel(q_steps, ha, hb, gain, cos, sin, wq, wk, wv, n_out, inv_out, q_out, k_out, v_out, ns, ws, sem, wsem):
    step = pl.program_id(0)
    half, width = ha.shape
    nk = wk.shape[1]
    blk = ws.shape[2]
    slots = ws.shape[0]
    save_n = pltpu.make_async_copy(ns, n_out, sem.at[4])
    load_kv = [pltpu.make_async_copy(w, ws.at[q_steps % slots, :, pl.ds(i * nk, nk)], sem.at[2 + i]) for i, w in enumerate((wk, wv))]

    def load_q(i):
        return pltpu.make_async_copy(wq.at[:, pl.ds(pl.multiple_of(i * blk, blk), blk)], ws.at[i % slots], wsem.at[i % slots])

    @pl.when(step == 0)
    def _():
        loads = [pltpu.make_async_copy(ha, ns.at[pl.ds(0, half)], sem.at[0]),
                 pltpu.make_async_copy(hb, ns.at[pl.ds(half, half)], sem.at[1])]
        for c in loads:
            c.start()
        for c in loads:
            c.wait()
        load_q(0).start()
        wide = 512

        def rows(i, _):
            at = pl.ds(pl.multiple_of(i * 48, 48), 48)
            total = jnp.zeros((48, wide), F32)
            for c in range(0, width, wide):
                x = ns[at, c:c + wide].astype(F32)
                total = total + x * x
            inv = lax.rsqrt(jnp.sum(total, axis=-1, keepdims=True) / width + NORM_EPS)
            for c in range(0, width, wide):
                x = ns[at, c:c + wide].astype(F32)
                ns[at, c:c + wide] = (x * inv * gain[:, c:c + wide]).astype(BF16)
            inv_out[at, :] = jnp.broadcast_to(inv, (48, 128))
            return 0

        chunks = 2 * half // 48
        lax.fori_loop(0, chunks // 2, rows, 0)
        load_q(1).start()
        lax.fori_loop(chunks // 2, chunks, rows, 0)
        load_q(2).start()

    @pl.when((step > 0) & (step + slots - 1 < q_steps))
    def _():
        load_q(step + slots - 1).start()

    @pl.when(step + slots - 1 == q_steps)
    def _():
        for c in load_kv:
            c.start()
        save_n.start()

    def rotated(raw):
        parts = []
        for j in range(raw.shape[1] // HEAD_DIM):
            x = raw[:, j * HEAD_DIM:(j + 1) * HEAD_DIM]
            parts.append((x * cos[...] + swap_pairs(x) * sin[...]).astype(BF16))
        return jnp.concatenate(parts, axis=1)

    @pl.when(step < q_steps)
    def _():
        load_q(step).wait()
        q_out[...] = rotated(dot(ns[...], ws[step % slots]))

    @pl.when(step == q_steps)
    def _():
        for c in load_kv:
            c.wait()
        r = dot(ns[...], ws[q_steps % slots])
        k_out[...] = rotated(r[:, :nk])
        v_out[...] = r[:, nk:].astype(BF16)
        save_n.wait()


def qkv(ha, hb, gain, cos, sin, wq, wk, wv):
    half, width = ha.shape
    tok = 2 * half
    nq, nk = wq.shape[1], wk.shape[1]
    blk = 2 * nk
    q_steps = nq // blk
    return pl.pallas_call(
        functools.partial(qkv_kernel, q_steps), name="qkv", grid=(q_steps + 1,),
        in_specs=[ANY, ANY, const_spec((1, width)), const_spec((tok, HEAD_DIM)), const_spec((tok, HEAD_DIM)), ANY, ANY, ANY],
        out_specs=[ANY, const_spec((tok, 128)),
                   pl.BlockSpec((tok, blk), lambda i: (0, jnp.minimum(i, q_steps - 1))),
                   const_spec((tok, nk)), const_spec((tok, nk))],
        out_shape=[jax.ShapeDtypeStruct((tok, width), BF16), jax.ShapeDtypeStruct((tok, 128), F32),
                   jax.ShapeDtypeStruct((tok, nq), BF16), jax.ShapeDtypeStruct((tok, nk), BF16),
                   jax.ShapeDtypeStruct((tok, nk), BF16)],
        scratch_shapes=[pltpu.VMEM((tok, width), BF16), pltpu.VMEM((3, width, blk), BF16), pltpu.SemaphoreType.DMA((5,)),
                        pltpu.SemaphoreType.DMA((3,))],
        compiler_params=params(62), cost_estimate=cost(2 * tok * width * (nq + 2 * nk), 2 * width * (nq + 2 * nk)),
    )(ha, hb, gain, cos, sin, wq, wk, wv)


def heads_grad_kernel(steps, ga, gb, w, *refs):
    out, gs, ws, sem, wsem = refs[-5:]
    step = pl.program_id(0)
    half = ga.shape[0]
    slots, blk = ws.shape[:2]

    def load(i):
        return pltpu.make_async_copy(w.at[pl.ds(pl.multiple_of(i * blk, blk), blk)], ws.at[i % slots], wsem.at[i % slots])

    @pl.when(step == 0)
    def _():
        loads = [pltpu.make_async_copy(ga, gs.at[pl.ds(0, half)], sem.at[0]),
                 pltpu.make_async_copy(gb, gs.at[pl.ds(half, half)], sem.at[1])]
        for c in loads:
            c.start()
        load(0).start()
        for c in loads:
            c.wait()
        for i in range(1, slots):
            load(i).start()

    @pl.when((step > 0) & (step + slots - 1 < steps))
    def _():
        load(step + slots - 1).start()

    load(step).wait()
    out[...] = dot(gs[...], ws[step % slots], NT).astype(BF16)


def heads_grad(ga, gb, w_out, *before):
    half, width = ga.shape
    tok = 2 * half
    n = w_out.shape[0]
    blk = 256
    steps = n // blk
    return pl.pallas_call(
        functools.partial(heads_grad_kernel, steps), name="heads_grad", grid=(steps,),
        in_specs=[ANY] * (3 + len(before)), out_specs=pl.BlockSpec((tok, blk), lambda i: (0, i)),
        out_shape=jax.ShapeDtypeStruct((tok, n), BF16),
        scratch_shapes=[pltpu.VMEM((tok, width), BF16), pltpu.VMEM((4, blk, width), BF16), pltpu.SemaphoreType.DMA((2,)),
                        pltpu.SemaphoreType.DMA((4,))],
        compiler_params=params(62), cost_estimate=cost(2 * tok * width * n, 2 * width * n),
    )(ga, gb, w_out, *before)


def by_head(a_ref, b_ref, group):
    def flat(r):
        v = r[...]
        return v.reshape(v.shape[0] * v.shape[2], v.shape[3])

    full = jnp.concatenate([flat(a_ref), flat(b_ref)], axis=0)
    return jnp.concatenate([full[:, h * HEAD_DIM:(h + 1) * HEAD_DIM] for h in range(group)], axis=0)


def put(ref, value):
    ref[...] = value.reshape(ref.shape)


def soft_weights(k, q, down, across):
    allowed = (down[0][:, 0:1] == across[0][0:1, :]) & (down[0][:, 1:2] <= across[0][1:2, :])
    scores = jnp.where(allowed, dot(k, q, NT), -1e30)
    e = jnp.exp2((scores - jnp.max(scores, axis=0, keepdims=True)) * (HEAD_DIM ** -0.5 * LOG2_E))
    return e, 1.0 / jnp.sum(e, axis=0, keepdims=True)


def attend_kernel(group, qa, qb, ka, kb, va, vb, down, across, out):
    q = by_head(qa, qb, group)
    k = by_head(ka, kb, 1)
    v = by_head(va, vb, 1)
    seq = k.shape[0]
    e, scale = soft_weights(k, q, down, across)
    o = dot((e * scale).astype(BF16), v, TN).astype(BF16)
    o = jnp.concatenate([o[h * seq:(h + 1) * seq] for h in range(group)], axis=1)
    put(out, o)


def head_specs(slots, rows, wide):
    return pl.BlockSpec((slots, 1, rows, wide), lambda r, h: (0, r, 0, h))


def mask_specs(seq, group):
    return [pl.BlockSpec((1, seq, 2), lambda r, h: (r, 0, 0)), pl.BlockSpec((1, 2, group * seq), lambda r, h: (r, 0, 0))]


def attend(qa, qb, ka, kb, va, vb, down, across):
    slots, batch, rows, nq = qa.shape
    kv = ka.shape[3] // HEAD_DIM
    group = nq // ka.shape[3]
    seq = 2 * slots * rows
    qs, ks = head_specs(slots, rows, group * HEAD_DIM), head_specs(slots, rows, HEAD_DIM)
    return pl.pallas_call(
        functools.partial(attend_kernel, group), name="attend", grid=(batch, kv),
        in_specs=[qs, qs, ks, ks, ks, ks] + mask_specs(seq, group),
        out_specs=head_specs(2 * slots, rows, group * HEAD_DIM),
        out_shape=jax.ShapeDtypeStruct((2 * slots,) + qa.shape[1:], BF16),
        compiler_params=params(62, "arbitrary", "arbitrary"),
        cost_estimate=cost(batch * kv * group * seq * seq * HEAD_DIM * 40, 4 * qa.size * 2),
    )(qa, qb, ka, kb, va, vb, down, across)


def attend_back_kernel(group, qa, qb, ka, kb, va, vb, ga, gb, down, across, ca, cb, sa, sb, dq_out, dk_out, dv_out):
    q = by_head(qa, qb, group)
    g = by_head(ga, gb, group)
    k = by_head(ka, kb, 1)
    v = by_head(va, vb, 1)
    cos, sin = by_head(ca, cb, 1) * HEAD_DIM ** -0.5, by_head(sa, sb, 1) * HEAD_DIM ** -0.5
    seq = k.shape[0]
    e, scale = soft_weights(k, q, down, across)
    probs = e * scale
    gp = dot(v, g, NT)
    dots = jnp.sum(probs * gp, axis=0, keepdims=True)
    ds = (probs * (gp - dots)).astype(BF16)
    dv = dot(probs.astype(BF16), g).astype(BF16)
    dk = dot(ds, q)
    dq = dot(ds, k, TN)

    def unrotated(x):
        return (x * cos - swap_pairs(x) * sin).astype(BF16)

    dq = jnp.concatenate([unrotated(dq[h * seq:(h + 1) * seq]) for h in range(group)], axis=1)
    dk = unrotated(dk)
    put(dq_out, dq)
    put(dk_out, dk)
    put(dv_out, dv)


def attend_back(qa, qb, ka, kb, va, vb, ga, gb, down, across, ca, cb, sa, sb):
    slots, batch, rows, nq = qa.shape
    kv = ka.shape[3] // HEAD_DIM
    group = nq // ka.shape[3]
    seq = 2 * slots * rows
    qs, ks = head_specs(slots, rows, group * HEAD_DIM), head_specs(slots, rows, HEAD_DIM)
    ts = pl.BlockSpec((slots, 1, rows, HEAD_DIM), lambda r, h: (0, r, 0, 0))
    return pl.pallas_call(
        functools.partial(attend_back_kernel, group), name="attend_back", grid=(batch, kv),
        in_specs=[qs, qs, ks, ks, ks, ks, qs, qs] + mask_specs(seq, group) + [ts, ts, ts, ts],
        out_specs=[head_specs(2 * slots, rows, wide) for wide in (group * HEAD_DIM, HEAD_DIM, HEAD_DIM)],
        out_shape=[jax.ShapeDtypeStruct((2 * slots,) + x.shape[1:], BF16) for x in (qa, ka, va)],
        compiler_params=params(62, "arbitrary", "arbitrary"),
        cost_estimate=cost(batch * kv * group * seq * seq * HEAD_DIM * 60, 8 * qa.size * 2),
    )(qa, qb, ka, kb, va, vb, ga, gb, down, across, ca, cb, sa, sb)


def out_share_kernel(o, w, *outs):
    r = dot(o[...], w[...])
    rows = outs[0].shape[0]
    for i, out in enumerate(outs):
        out[...] = r[i * rows:(i + 1) * rows].astype(out.dtype)


def out_share(o, w_out, types):
    tok, n = o.shape
    width = w_out.shape[1]
    blk = 1024
    rows = tok // len(types)
    return pl.pallas_call(
        out_share_kernel, name="out_share", grid=(width // blk,),
        in_specs=[const_spec((tok, n)), pl.BlockSpec((n, blk), lambda i: (0, i))],
        out_specs=[pl.BlockSpec((rows, blk), lambda i: (0, i))] * len(types),
        out_shape=[jax.ShapeDtypeStruct((rows, width), t) for t in types],
        compiler_params=params(62), cost_estimate=cost(2 * tok * width * n, 2 * width * n),
    )(o, w_out)


def norm_share_kernel(dq, dk, dv, wq, wk, wv, h0, h1, h2, h3, inv_a, inv_b, d0, d1, d2, d3, gain):
    r = dot(dq[...], wq[...], NT) + dot(dk[...], wk[...], NT) + dot(dv[...], wv[...], NT)
    rows = d0.shape[0]
    total = 0.0
    for i, (h, d) in enumerate(((h0, d0), (h1, d1), (h2, d2), (h3, d3))):
        part = r[i * rows:(i + 1) * rows]
        d[...] = part.astype(d.dtype)
        inv = (inv_a, inv_b)[i // 2][(i % 2) * rows:(i % 2 + 1) * rows, :1]
        total = total + jnp.sum(part * (h[...].astype(F32) * inv), axis=0, keepdims=True)
    gain[...] = total


def norm_share(dq, dk, dv, wq, wk, wv, h, inv_a, inv_b):
    tok, nq = dq.shape
    nk = dk.shape[1]
    width = wq.shape[0]
    blk = 1024
    spec = pl.BlockSpec((tok // 4, blk), lambda i: (0, i))
    return pl.pallas_call(
        norm_share_kernel, name="norm_share", grid=(width // blk,),
        in_specs=[const_spec((tok, nq)), const_spec((tok, nk)), const_spec((tok, nk)),
                  pl.BlockSpec((blk, nq), lambda i: (i, 0)), pl.BlockSpec((blk, nk), lambda i: (i, 0)),
                  pl.BlockSpec((blk, nk), lambda i: (i, 0)), spec, spec, spec, spec,
                  const_spec((tok // 2, 128)), const_spec((tok // 2, 128))],
        out_specs=[spec] * 4 + [pl.BlockSpec((1, blk), lambda i: (0, i))],
        out_shape=[jax.ShapeDtypeStruct((tok // 4, width), BF16)] * 4 + [jax.ShapeDtypeStruct((1, width), F32)],
        compiler_params=params(62), cost_estimate=cost(2 * tok * width * (nq + 2 * nk), 2 * width * (nq + 2 * nk)),
    )(dq, dk, dv, wq, wk, wv, *h, inv_a, inv_b)


def weight_grads_kernel(steps, na, nb, dq, dk, dv, o, g0, g1, g2, g3, p0, p1, p2, h, gq, gk, gv, g_out, out, ot):
    step = pl.program_id(0)

    @pl.when(step < steps)
    def _():
        n = jnp.concatenate([na[...], nb[...]], axis=0).T
        for d, grad in ((dq, gq), (dk, gk), (dv, gv)):
            grad[...] = dot(n, d[...])

    @pl.when(step == steps)
    def _():
        for c in range(0, o.shape[1], 256):
            ot[c:c + 256, :] = o[:, c:c + 256].T

    @pl.when(step >= steps)
    def _():
        g_out[...] = dot(ot[...], jnp.concatenate([g0[...], g1[...], g2[...], g3[...]], axis=0))
        share = sum(x[...].astype(F32) for x in (p0, p1, p2))
        out[...] = (h[...].astype(F32) + share.astype(BF16).astype(F32)).astype(BF16)


def weight_grads(na, nb, dq, dk, dv, o, g, p, h):
    tok, nq = dq.shape
    nk = dk.shape[1]
    width = na.shape[1]
    blk = 1024
    steps = width // blk

    def early(i):
        return jnp.minimum(i, steps - 1)

    def late(i):
        return jnp.maximum(i - steps, 0)

    rows = pl.BlockSpec((tok // 4, blk), lambda i: (0, late(i)))
    return pl.pallas_call(
        functools.partial(weight_grads_kernel, steps), name="weight_grads", grid=(2 * steps,),
        in_specs=[pl.BlockSpec((tok // 2, blk), lambda i: (0, early(i)))] * 2 + [const_spec((tok, nq))] + [const_spec((tok, nk))] * 2
        + [const_spec((tok, nq))] + [rows] * 8,
        out_specs=[pl.BlockSpec((blk, n), lambda i: (early(i), 0)) for n in (nq, nk, nk)] + [pl.BlockSpec((nq, blk), lambda i: (0, late(i))), rows],
        out_shape=[jax.ShapeDtypeStruct((width, n), F32) for n in (nq, nk, nk)]
        + [jax.ShapeDtypeStruct((nq, width), F32), jax.ShapeDtypeStruct(h.shape, BF16)],
        scratch_shapes=[pltpu.VMEM((nq, tok), BF16)],
        compiler_params=params(62), cost_estimate=cost(4 * tok * width * (nq + nk), 8 * width * (nq + nk)),
    )(na, nb, dq, dk, dv, o, *g, *p, h)


def norm_back_kernel(d0, d1, d2, h, g, inv, gain, grad, dg):
    rows, width = h.shape
    wide = 1024
    total = jnp.zeros((rows, wide), F32)
    for c in range(0, width, wide):
        at = slice(c, c + wide)
        x = sum(d[:, at].astype(F32) for d in (d0, d1, d2)) * gain[:, at]
        dg[:, at] = x
        total = total + x * h[:, at].astype(F32)
    s = inv[:, :1]
    back = (s * s * s) * (jnp.sum(total, axis=-1, keepdims=True) / width)
    s = jnp.broadcast_to(s, (rows, wide))
    back = jnp.broadcast_to(back, (rows, wide))
    for c in range(0, width, wide):
        at = slice(c, c + wide)
        grad[:, at] = (g[:, at].astype(F32) + (s * dg[:, at] - h[:, at].astype(F32) * back)).astype(BF16)


def norm_back(d, h, g, inv, gain):
    tok, width = h.shape
    blk = 48
    spec = pl.BlockSpec((blk, width), lambda i: (i, 0))
    return pl.pallas_call(
        norm_back_kernel, name="norm_back", grid=(tok // blk,),
        in_specs=[spec] * 5 + [pl.BlockSpec((blk, 128), lambda i: (i, 0)), const_spec((1, width))],
        out_specs=spec, out_shape=jax.ShapeDtypeStruct((tok, width), BF16), scratch_shapes=[pltpu.VMEM((blk, width), F32)],
        compiler_params=params(62), cost_estimate=cost(20 * tok * width, 12 * tok * width),
    )(*d, h, g, inv, gain)


def solution(mesh):
    tp_size = mesh.shape['tp']
    beside = [(i, i ^ 1) for i in range(tp_size)]
    across = [(i, i ^ 2) for i in range(tp_size)]
    diagonal = [(i, i ^ 3) for i in range(tp_size)]

    def send(x, pairs):
        return lax.ppermute(x, 'tp', pairs)

    def after(x, *others):
        return lax.optimization_barrier((x,) + others)[0]

    def step(hidden, positions, doc_ids, norm_gain, w_query, w_key, w_value, w_out, grad_out):
        batch, rows, width = hidden.shape
        tok = batch * rows
        nq, nk = w_query.shape[1], w_key.shape[1]
        group = nq // nk
        gain = norm_gain.astype(F32).reshape(1, width)

        pos1, doc1 = send(positions, beside), send(doc_ids, beside)
        pos2, doc2 = send(positions, across), send(doc_ids, across)
        h0 = hidden.reshape(tok, width)
        g0 = grad_out.reshape(tok, width)
        h2 = send(h0, across)
        h1 = send(h0, beside)
        g1 = send(g0, beside)
        g2 = send(g0, across)
        h3 = send(h2, beside)

        lane = jnp.arange(HEAD_DIM)
        inv_freq = ROPE_BASE ** (-(lane // 2 * 2).astype(F32) / HEAD_DIM)
        sign = jnp.where(lane % 2 == 0, -1.0, 1.0)

        def tables(*pos):
            angles = jnp.stack(pos).astype(F32)[..., None] * inv_freq
            return jnp.cos(angles), jnp.sin(angles) * sign

        def heads(x):
            return x.reshape(2, batch, rows, x.shape[1])

        def flat(x):
            return x.reshape(x.shape[0] * tok, x.shape[3])

        ca, sa = tables(positions, pos1)
        na, inv_a, qa, ka, va = qkv(h0, h1, gain, ca.reshape(2 * tok, HEAD_DIM), sa.reshape(2 * tok, HEAD_DIM), w_query, w_key, w_value)
        pos2, doc2, ka = lax.optimization_barrier((pos2, doc2, ka))
        pos3, doc3 = send(pos2, beside), send(doc2, beside)
        cb, sb = tables(pos2, pos3)
        both = jnp.stack([jnp.concatenate([doc_ids, doc1, doc2, doc3], axis=1), jnp.concatenate([positions, pos1, pos2, pos3], axis=1)], axis=1)
        down, over = jnp.swapaxes(both, 1, 2), jnp.tile(both, (1, 1, group))
        dha = heads_grad(g0, g1, w_out, ka, cb, sb, down, over)
        nb, inv_b, qb, kb, vb = qkv(h2, h3, gain, cb.reshape(2 * tok, HEAD_DIM), sb.reshape(2 * tok, HEAD_DIM), w_query, w_key, w_value)
        saved = [heads(x) for x in (qa, qb, ka, kb, va, vb)]
        o = flat(attend(*saved, down, over))

        p0, p1, p2, p3 = out_share(o, w_out, (BF16, BF16, F32, BF16))
        g3 = send(after(g2, p2), beside)
        p3 = send(p3, beside)
        p1 = send(p1, beside)
        dhb = heads_grad(g2, g3, w_out)
        s2 = (p2 + after(p3, dhb).astype(F32)).astype(BF16)
        s2, dhb = lax.optimization_barrier((s2, dhb))
        s2 = send(s2, across)
        grads = attend_back(*saved, heads(dha), heads(dhb), down, over, ca, cb, sa, sb)
        dq, dk, dv = [flat(x) for x in grads]
        d0, d1, d2, d3, gg = norm_share(dq, dk, dv, w_query, w_key, w_value, (h0, h1, h2, h3), inv_a, inv_b)
        d3 = send(d3, beside)
        d1 = send(d1, beside)
        t2 = (d2.astype(F32) + d3.astype(F32)).astype(BF16)
        t2, gg, dq = lax.optimization_barrier((t2, gg, dq))
        t2 = send(t2, across)
        gg1, gg2, gg3 = send(gg, beside), send(gg, across), send(gg, diagonal)
        gq, gk, gv, g_out, attn_out = weight_grads(na, nb, dq, dk, dv, o, (g0, g1, g2, g3), (p0, p1, s2), h0)
        grad_hidden = norm_back((after(d0, gk), d1, t2), h0, g0, inv_a, gain)
        grad_gain = ((gg + gg1) + (gg2 + gg3)).reshape(width)
        attn_out, grad_hidden = attn_out.reshape(hidden.shape), grad_hidden.reshape(hidden.shape)
        return (attn_out, grad_hidden, grad_gain, gq, gk, gv, g_out)

    row_spec = P('dp', 'tp', None)
    tok_spec = P('dp', 'tp')
    col_spec = P(None, 'tp')

    return jax.shard_map(
        step, mesh=mesh,
        in_specs=(row_spec, tok_spec, tok_spec, P(), col_spec, col_spec, col_spec, P('tp', None), row_spec),
        out_specs=(row_spec, row_spec, P('dp'), P('dp', 'tp'), P('dp', 'tp'), P('dp', 'tp'), P(('dp', 'tp'), None)),
        check_vma=False)
```

```python
import functools

import jax
import jax.numpy as jnp
from jax import lax
from jax.experimental import pallas as pl
from jax.experimental.pallas import tpu as pltpu
from jax.sharding import PartitionSpec as P


HEAD_DIM = 128
NORM_EPS = 1e-5
ROPE_BASE = 10000.0
LOG2_E = 1.4426950408889634
BF16 = jnp.bfloat16
F32 = jnp.float32
ANY = pl.BlockSpec(memory_space=pl.ANY)
NN = (((1,), (0,)), ((), ()))
NT = (((1,), (1,)), ((), ()))
TN = (((0,), (0,)), ((), ()))


def dot(a, b, dims=NN):
    return lax.dot_general(a, b, dims, preferred_element_type=F32)


def const_spec(shape):
    return pl.BlockSpec(shape, lambda *_: (0,) * len(shape), pipeline_mode=pl.Buffered(1))


def params(mib, *semantics):
    return pltpu.CompilerParams(dimension_semantics=semantics or ("arbitrary",), vmem_limit_bytes=mib << 20)


def cost(flops, moved):
    return pl.CostEstimate(flops=int(flops), bytes_accessed=int(moved), transcendentals=0)


def swap_pairs(x):
    lane = lax.broadcasted_iota(jnp.int32, x.shape, x.ndim - 1)
    return jnp.where(lane % 2 == 0, pltpu.roll(x, x.shape[-1] - 1, x.ndim - 1), pltpu.roll(x, 1, x.ndim - 1))


def project(step, ha, hb, gain, cos, sin, wq, wk, wv, n_out, inv_out, q_out, k_out, v_out, ns, ws, sem, wsem):
    half, width = ha.shape
    nk = wk.shape[1]
    slots, _, blk = ws.shape
    q_steps = wq.shape[1] // blk
    save_n = pltpu.make_async_copy(ns, n_out, sem.at[4])
    load_kv = [pltpu.make_async_copy(w, ws.at[q_steps % slots, :, pl.ds(i * nk, nk)], sem.at[2 + i]) for i, w in enumerate((wk, wv))]

    def load_q(i):
        return pltpu.make_async_copy(wq.at[:, pl.ds(pl.multiple_of(i * blk, blk), blk)], ws.at[i % slots], wsem.at[i % slots])

    @pl.when(step == 0)
    def _():
        loads = [pltpu.make_async_copy(ha, ns.at[pl.ds(0, half)], sem.at[0]),
                 pltpu.make_async_copy(hb, ns.at[pl.ds(half, half)], sem.at[1])]
        for c in loads:
            c.start()
        for c in loads:
            c.wait()
        load_q(0).start()
        wide = 512

        def rows(i, _):
            at = pl.ds(pl.multiple_of(i * 48, 48), 48)
            total = jnp.zeros((48, wide), F32)
            for c in range(0, width, wide):
                x = ns[at, c:c + wide].astype(F32)
                total = total + x * x
            inv = lax.rsqrt(jnp.sum(total, axis=-1, keepdims=True) / width + NORM_EPS)
            for c in range(0, width, wide):
                x = ns[at, c:c + wide].astype(F32)
                ns[at, c:c + wide] = (x * inv * gain[:, c:c + wide]).astype(BF16)
            inv_out[at, :] = jnp.broadcast_to(inv, (48, 128))
            return 0

        chunks = 2 * half // 48
        lax.fori_loop(0, chunks // 2, rows, 0)
        load_q(1).start()
        lax.fori_loop(chunks // 2, chunks, rows, 0)
        load_q(2).start()

    @pl.when((step > 0) & (step + slots - 1 < q_steps))
    def _():
        load_q(step + slots - 1).start()

    @pl.when(step + slots - 1 == q_steps)
    def _():
        for c in load_kv:
            c.start()
        save_n.start()

    def rotated(raw):
        parts = []
        for j in range(raw.shape[1] // HEAD_DIM):
            x = raw[:, j * HEAD_DIM:(j + 1) * HEAD_DIM]
            parts.append((x * cos[...] + swap_pairs(x) * sin[...]).astype(BF16))
        return jnp.concatenate(parts, axis=1)

    @pl.when(step < q_steps)
    def _():
        load_q(step).wait()
        q_out[:, pl.ds(pl.multiple_of(step * blk, blk), blk)] = rotated(dot(ns[...], ws[step % slots]))

    @pl.when(step == q_steps)
    def _():
        for c in load_kv:
            c.wait()
        r = dot(ns[...], ws[q_steps % slots])
        k_out[...] = rotated(r[:, :nk])
        v_out[...] = r[:, nk:].astype(BF16)
        save_n.wait()


def project_out(tok, width, nq, nk):
    shapes = [jax.ShapeDtypeStruct((tok, 128), F32)] + [jax.ShapeDtypeStruct((tok, n), BF16) for n in (nq, nk, nk)]
    return [ANY] + [const_spec(x.shape) for x in shapes], [jax.ShapeDtypeStruct((tok, width), BF16)] + shapes


def project_scratch(tok, width, blk):
    return [pltpu.VMEM((tok, width), BF16), pltpu.VMEM((3, width, blk), BF16), pltpu.SemaphoreType.DMA((5,)), pltpu.SemaphoreType.DMA((3,))]


def qkv(ha, hb, gain, cos, sin, wq, wk, wv):
    half, width = ha.shape
    tok = 2 * half
    nq, nk = wq.shape[1], wk.shape[1]
    blk = 2 * nk
    specs, shapes = project_out(tok, width, nq, nk)
    return pl.pallas_call(
        lambda *refs: project(pl.program_id(0), *refs), name="qkv", grid=(nq // blk + 1,),
        in_specs=[ANY, ANY, const_spec((1, width)), const_spec((tok, HEAD_DIM)), const_spec((tok, HEAD_DIM)), ANY, ANY, ANY],
        out_specs=specs, out_shape=shapes, scratch_shapes=project_scratch(tok, width, blk),
        compiler_params=params(62), cost_estimate=cost(2 * tok * width * (nq + 2 * nk), 2 * width * (nq + 2 * nk)),
    )(ha, hb, gain, cos, sin, wq, wk, wv)


def heads_grad_kernel(steps, ga, gb, w, *refs):
    out, gs, ws, sem, wsem = refs[-5:]
    step = pl.program_id(0)
    half = ga.shape[0]
    slots, blk = ws.shape[:2]

    def load(i):
        return pltpu.make_async_copy(w.at[pl.ds(pl.multiple_of(i * blk, blk), blk)], ws.at[i % slots], wsem.at[i % slots])

    @pl.when(step == 0)
    def _():
        loads = [pltpu.make_async_copy(ga, gs.at[pl.ds(0, half)], sem.at[0]),
                 pltpu.make_async_copy(gb, gs.at[pl.ds(half, half)], sem.at[1])]
        for c in loads:
            c.start()
        load(0).start()
        for c in loads:
            c.wait()
        for i in range(1, slots):
            load(i).start()

    @pl.when((step > 0) & (step + slots - 1 < steps))
    def _():
        load(step + slots - 1).start()

    load(step).wait()
    out[...] = dot(gs[...], ws[step % slots], NT).astype(BF16)


def heads_grad(ga, gb, w_out, *before):
    half, width = ga.shape
    tok = 2 * half
    n = w_out.shape[0]
    blk = 256
    steps = n // blk
    return pl.pallas_call(
        functools.partial(heads_grad_kernel, steps), name="heads_grad", grid=(steps,),
        in_specs=[ANY] * (3 + len(before)), out_specs=pl.BlockSpec((tok, blk), lambda i: (0, i)),
        out_shape=jax.ShapeDtypeStruct((tok, n), BF16),
        scratch_shapes=[pltpu.VMEM((tok, width), BF16), pltpu.VMEM((4, blk, width), BF16), pltpu.SemaphoreType.DMA((2,)),
                        pltpu.SemaphoreType.DMA((4,))],
        compiler_params=params(62), cost_estimate=cost(2 * tok * width * n, 2 * width * n),
    )(ga, gb, w_out, *before)


def tokens_of(refs, row, rows, batch):
    parts = []
    for ref in refs:
        for block in range(ref.shape[0] // (batch * rows)):
            parts.append(ref[pl.ds(pl.multiple_of((block * batch + row) * rows, rows), rows), :])
    return jnp.concatenate(parts, axis=0)


def put_tokens(ref, row, rows, batch, lanes, value):
    for block in range(ref.shape[0] // (batch * rows)):
        ref[pl.ds(pl.multiple_of((block * batch + row) * rows, rows), rows), lanes] = value[block * rows:(block + 1) * rows]


def heads_down(x):
    return jnp.concatenate([x[:, c:c + HEAD_DIM] for c in range(0, x.shape[1], HEAD_DIM)], axis=0)


def heads_across(x, seq):
    return jnp.concatenate([x[c:c + seq] for c in range(0, x.shape[0], seq)], axis=1)


def soft_weights(k, q, down, across):
    allowed = (down[:, 0:1] == across[0:1, :]) & (down[:, 1:2] <= across[1:2, :])
    scores = jnp.where(allowed, dot(k, q, NT), -1e30)
    e = jnp.exp2((scores - jnp.max(scores, axis=0, keepdims=True)) * (HEAD_DIM ** -0.5 * LOG2_E))
    return e, 1.0 / jnp.sum(e, axis=0, keepdims=True)


def attend_row(row, rows, batch, q_refs, k_refs, v_refs, down, across, out):
    q, k, v = (tokens_of(r, row, rows, batch) for r in (q_refs, k_refs, v_refs))
    wide = HEAD_DIM * (q.shape[1] // k.shape[1])
    for i in range(k.shape[1] // HEAD_DIM):
        at, kv = slice(i * wide, (i + 1) * wide), slice(i * HEAD_DIM, (i + 1) * HEAD_DIM)
        e, scale = soft_weights(k[:, kv], heads_down(q[:, at]), down[row], across[row])
        o = dot((e * scale).astype(BF16), v[:, kv], TN).astype(BF16)
        put_tokens(out, row, rows, batch, at, heads_across(o, k.shape[0]))


def attend_back_row(row, rows, batch, q_refs, k_refs, v_refs, g_refs, down, across, cos_refs, sin_refs, dq_out, dk_out, dv_out):
    q, k, v, g = (tokens_of(r, row, rows, batch) for r in (q_refs, k_refs, v_refs, g_refs))
    cos, sin = (tokens_of(r, row, rows, batch) * HEAD_DIM ** -0.5 for r in (cos_refs, sin_refs))
    seq = k.shape[0]
    wide = HEAD_DIM * (q.shape[1] // k.shape[1])

    def unrotated(x):
        return (x * cos - swap_pairs(x) * sin).astype(BF16)

    for i in range(k.shape[1] // HEAD_DIM):
        at, kv = slice(i * wide, (i + 1) * wide), slice(i * HEAD_DIM, (i + 1) * HEAD_DIM)
        qh, gh = heads_down(q[:, at]), heads_down(g[:, at])
        e, scale = soft_weights(k[:, kv], qh, down[row], across[row])
        probs = e * scale
        gp = dot(v[:, kv], gh, NT)
        ds = (probs * (gp - jnp.sum(probs * gp, axis=0, keepdims=True))).astype(BF16)
        put_tokens(dv_out, row, rows, batch, kv, dot(probs.astype(BF16), gh).astype(BF16))
        put_tokens(dk_out, row, rows, batch, kv, unrotated(dot(ds, qh)))
        dq = dot(ds, k[:, kv], TN)
        dq = jnp.concatenate([unrotated(dq[c:c + seq]) for c in range(0, dq.shape[0], seq)], axis=1)
        put_tokens(dq_out, row, rows, batch, at, dq)


def chip_sum(first, steps, share, out, keep, box, got, send_sem, recv_sem):
    now = pl.program_id(0)
    step = now - first
    tp = lax.axis_index("tp")
    neighbour = {"tp": tp + 1 - 2 * lax.rem(tp, 2)}

    def copy(i):
        return pltpu.make_async_remote_copy(box.at[i % 2], got.at[i % 2], send_sem.at[i % 2], recv_sem.at[i % 2],
                                            device_id=neighbour, device_id_type=pl.DeviceIdType.MESH)

    @pl.when(now == 0)
    def _():
        barrier = pltpu.get_barrier_semaphore()
        pl.semaphore_signal(barrier, inc=1, device_id=neighbour, device_id_type=pl.DeviceIdType.MESH)
        pl.semaphore_wait(barrier, 1)

    @pl.when(step > 0)
    def _():
        copy(step - 1).start()

    @pl.when((step >= 0) & (step < steps))
    def _():
        counterpart, diagonal = share()
        keep[step % 2] = counterpart
        box[step % 2] = diagonal

    @pl.when(step > 0)
    def _():
        copy(step - 1).wait()
        out[...] = (keep[(step - 1) % 2] + got[(step - 1) % 2]).astype(BF16)


def chip_sum_scratch(rows, blk):
    return [pltpu.VMEM((2, rows, blk), F32)] * 3 + [pltpu.SemaphoreType.DMA((2,))] * 2


def clip(i, n):
    return jnp.clip(i, 0, n - 1)


def comm_params(number):
    return pltpu.CompilerParams(dimension_semantics=("arbitrary",), vmem_limit_bytes=62 << 20, collective_id=number, has_side_effects=True)


def forward_kernel(batch, first, steps, ha, hb, gain, cos, sin, wq, wk, wv, qa, ka, va, down, across, w_out,
                   n_out, inv_out, qb, kb, vb, o, p0, p1, s2, ns, ws, sem, wsem, wo, osem, *chip):
    step = pl.program_id(0)
    slots, _, blk = wo.shape
    attend_at = first - batch

    def load(i):
        return pltpu.make_async_copy(w_out.at[:, pl.ds(pl.multiple_of(i * blk, blk), blk)], wo.at[i % slots], osem.at[i % slots])

    @pl.when(step < attend_at)
    def _():
        project(step, ha, hb, gain, cos, sin, wq, wk, wv, n_out, inv_out, qb, kb, vb, ns, ws, sem, wsem)

    @pl.when(step == attend_at - 1)
    def _():
        for i in range(slots):
            load(i).start()

    @pl.when((step >= attend_at) & (step < first))
    def _():
        rows = qa.shape[0] // (2 * batch)
        attend_row(step - attend_at, rows, batch, (qa, qb), (ka, kb), (va, vb), down, across, o)

    @pl.when((step > first) & (step - first + slots - 1 < steps))
    def _():
        load(step - first + slots - 1).start()

    def share():
        load(step - first).wait()
        r = dot(o[...], wo[(step - first) % slots])
        rows = p0.shape[0]
        p0[...] = r[:rows].astype(BF16)
        p1[...] = r[rows:2 * rows].astype(BF16)
        return r[2 * rows:3 * rows], r[3 * rows:]

    chip_sum(first, steps, share, s2, *chip)


def forward(batch, ha, hb, gain, cos, sin, wq, wk, wv, qa, ka, va, down, across, w_out):
    half, width = ha.shape
    tok = 2 * half
    nq, nk = wq.shape[1], wk.shape[1]
    wide, blk = 2 * nk, 1024
    first, steps = nq // wide + 1 + batch, width // blk
    specs, shapes = project_out(tok, width, nq, nk)
    now = pl.BlockSpec((half, blk), lambda i: (0, clip(i - first, steps)))
    late = pl.BlockSpec((half, blk), lambda i: (0, clip(i - first - 1, steps)))
    return pl.pallas_call(
        functools.partial(forward_kernel, batch, first, steps), name="forward", grid=(first + steps + 1,),
        in_specs=[ANY, ANY] + [const_spec(x.shape) for x in (gain, cos, sin)] + [ANY] * 3
        + [const_spec(x.shape) for x in (qa, ka, va, down, across)] + [ANY],
        out_specs=specs + [const_spec((2 * tok, nq)), now, now, late],
        out_shape=shapes + [jax.ShapeDtypeStruct((2 * tok, nq), BF16)] + [jax.ShapeDtypeStruct((half, width), BF16)] * 3,
        scratch_shapes=project_scratch(tok, width, wide) + [pltpu.VMEM((3, nq, blk), BF16), pltpu.SemaphoreType.DMA((3,))]
        + chip_sum_scratch(half, blk),
        compiler_params=comm_params(0), cost_estimate=cost(2 * tok * width * (3 * nq + 2 * nk), 4 * width * nq),
    )(ha, hb, gain, cos, sin, wq, wk, wv, qa, ka, va, down, across, w_out)


def backward_kernel(batch, heads_steps, steps, ga, gb, w_out, gh_a, qa, qb, ka, kb, va, vb, down, across, ca, cb, sa, sb,
                    wq, wk, wv, h0, h1, h2, h3, inv_a, inv_b,
                    dq, dk, dv, d0, d1, t2, gain, gs, gh_b, wo, ws, wks, wvs, sem, osem, wsem, *chip):
    step = pl.program_id(0)
    half = ga.shape[0]
    slots, blk = wo.shape[:2]
    w_slots, wide = ws.shape[:2]
    first = heads_steps + batch

    def load(i):
        return pltpu.make_async_copy(w_out.at[pl.ds(pl.multiple_of(i * blk, blk), blk)], wo.at[i % slots], osem.at[i % slots])

    def load_w(i):
        at = pl.ds(pl.multiple_of(i * wide, wide), wide)
        return [pltpu.make_async_copy(w.at[at], buf.at[i % w_slots], wsem.at[j, i % w_slots])
                for j, (w, buf) in enumerate(((wq, ws), (wk, wks), (wv, wvs)))]

    def start_w(i):
        for c in load_w(i):
            c.start()

    @pl.when(step == 0)
    def _():
        loads = [pltpu.make_async_copy(ga, gs.at[pl.ds(0, half)], sem.at[0]),
                 pltpu.make_async_copy(gb, gs.at[pl.ds(half, half)], sem.at[1])]
        for c in loads:
            c.start()
        load(0).start()
        for c in loads:
            c.wait()
        for i in range(1, slots):
            load(i).start()

    @pl.when((step > 0) & (step + slots - 1 < heads_steps))
    def _():
        load(step + slots - 1).start()

    @pl.when(step < heads_steps)
    def _():
        load(step).wait()
        gh_b[:, pl.ds(pl.multiple_of(step * blk, blk), blk)] = dot(gs[...], wo[step % slots], NT).astype(BF16)

    @pl.when(step == heads_steps - 1)
    def _():
        for i in range(w_slots):
            start_w(i)

    @pl.when((step >= heads_steps) & (step < first))
    def _():
        rows = qa.shape[0] // (2 * batch)
        attend_back_row(step - heads_steps, rows, batch, (qa, qb), (ka, kb), (va, vb), (gh_a, gh_b), down, across, (ca, cb), (sa, sb), dq, dk, dv)

    @pl.when((step > first) & (step - first + w_slots - 1 < steps))
    def _():
        start_w(step - first + w_slots - 1)

    def share():
        i = step - first
        for c in load_w(i):
            c.wait()
        i = i % w_slots
        r = dot(dq[...], ws[i], NT) + dot(dk[...], wks[i], NT) + dot(dv[...], wvs[i], NT)
        parts = [r[j * half:(j + 1) * half] for j in range(4)]
        d0[...] = parts[0].astype(BF16)
        d1[...] = parts[1].astype(BF16)
        total = 0.0
        for j, (part, h) in enumerate(zip(parts, (h0, h1, h2, h3))):
            inv = (inv_a, inv_b)[j // 2][(j % 2) * half:(j % 2 + 1) * half, :1]
            total = total + jnp.sum(part * (h[...].astype(F32) * inv), axis=0, keepdims=True)
        gain[...] = total
        return parts[2], parts[3]

    chip_sum(first, steps, share, t2, *chip)


def backward(batch, ga, gb, w_out, gh_a, qa, qb, ka, kb, va, vb, down, across, ca, cb, sa, sb, wq, wk, wv, h, inv_a, inv_b):
    half, width = ga.shape
    tok = 4 * half
    nq, nk = wq.shape[1], wk.shape[1]
    blk, wide = 256, 1024
    heads_steps, steps = nq // blk, width // wide
    first = heads_steps + batch
    now = pl.BlockSpec((half, wide), lambda i: (0, clip(i - first, steps)))
    late = pl.BlockSpec((half, wide), lambda i: (0, clip(i - first - 1, steps)))
    kept = (gh_a, qa, qb, ka, kb, va, vb, down, across, ca, cb, sa, sb)
    return pl.pallas_call(
        functools.partial(backward_kernel, batch, heads_steps, steps), name="backward", grid=(first + steps + 1,),
        in_specs=[ANY] * 3 + [const_spec(x.shape) for x in kept] + [ANY] * 3 + [now] * 4 + [const_spec(x.shape) for x in (inv_a, inv_b)],
        out_specs=[const_spec((tok, n)) for n in (nq, nk, nk)] + [now, now, late, pl.BlockSpec((1, wide), lambda i: (0, clip(i - first, steps)))],
        out_shape=[jax.ShapeDtypeStruct((tok, n), BF16) for n in (nq, nk, nk)] + [jax.ShapeDtypeStruct((half, width), BF16)] * 3
        + [jax.ShapeDtypeStruct((1, width), F32)],
        scratch_shapes=[pltpu.VMEM((2 * half, width), BF16), pltpu.VMEM((2 * half, nq), BF16), pltpu.VMEM((4, blk, width), BF16),
                        pltpu.VMEM((3, wide, nq), BF16), pltpu.VMEM((3, wide, nk), BF16), pltpu.VMEM((3, wide, nk), BF16),
                        pltpu.SemaphoreType.DMA((2,)), pltpu.SemaphoreType.DMA((4,)), pltpu.SemaphoreType.DMA((3, 3))]
        + chip_sum_scratch(half, wide),
        compiler_params=comm_params(1), cost_estimate=cost(2 * tok * width * (2 * nq + 2 * nk), 4 * width * nq),
    )(ga, gb, w_out, *kept, wq, wk, wv, *h, inv_a, inv_b)


def weight_grads_kernel(steps, na, nb, dq, dk, dv, o, g0, g1, g2, g3, p0, p1, p2, h, gq, gk, gv, g_out, out, ot):
    step = pl.program_id(0)

    @pl.when(step < steps)
    def _():
        n = jnp.concatenate([na[...], nb[...]], axis=0).T
        for d, grad in ((dq, gq), (dk, gk), (dv, gv)):
            grad[...] = dot(n, d[...])

    @pl.when(step == steps)
    def _():
        for c in range(0, o.shape[1], 256):
            ot[c:c + 256, :] = o[:, c:c + 256].T

    @pl.when(step >= steps)
    def _():
        g_out[...] = dot(ot[...], jnp.concatenate([g0[...], g1[...], g2[...], g3[...]], axis=0))
        share = sum(x[...].astype(F32) for x in (p0, p1, p2))
        out[...] = (h[...].astype(F32) + share.astype(BF16).astype(F32)).astype(BF16)


def weight_grads(na, nb, dq, dk, dv, o, g, p, h):
    tok, nq = dq.shape
    nk = dk.shape[1]
    width = na.shape[1]
    blk = 1024
    steps = width // blk

    def early(i):
        return jnp.minimum(i, steps - 1)

    def late(i):
        return jnp.maximum(i - steps, 0)

    rows = pl.BlockSpec((tok // 4, blk), lambda i: (0, late(i)))
    return pl.pallas_call(
        functools.partial(weight_grads_kernel, steps), name="weight_grads", grid=(2 * steps,),
        in_specs=[pl.BlockSpec((tok // 2, blk), lambda i: (0, early(i)))] * 2 + [const_spec((tok, nq))] + [const_spec((tok, nk))] * 2
        + [const_spec((tok, nq))] + [rows] * 8,
        out_specs=[pl.BlockSpec((blk, n), lambda i: (early(i), 0)) for n in (nq, nk, nk)] + [pl.BlockSpec((nq, blk), lambda i: (0, late(i))), rows],
        out_shape=[jax.ShapeDtypeStruct((width, n), F32) for n in (nq, nk, nk)]
        + [jax.ShapeDtypeStruct((nq, width), F32), jax.ShapeDtypeStruct(h.shape, BF16)],
        scratch_shapes=[pltpu.VMEM((nq, tok), BF16)],
        compiler_params=params(62), cost_estimate=cost(4 * tok * width * (nq + nk), 8 * width * (nq + nk)),
    )(na, nb, dq, dk, dv, o, *g, *p, h)


def norm_back_kernel(d0, d1, d2, h, g, inv, gain, grad, dg):
    rows, width = h.shape
    wide = 1024
    total = jnp.zeros((rows, wide), F32)
    for c in range(0, width, wide):
        at = slice(c, c + wide)
        x = sum(d[:, at].astype(F32) for d in (d0, d1, d2)) * gain[:, at]
        dg[:, at] = x
        total = total + x * h[:, at].astype(F32)
    s = inv[:, :1]
    back = (s * s * s) * (jnp.sum(total, axis=-1, keepdims=True) / width)
    s = jnp.broadcast_to(s, (rows, wide))
    back = jnp.broadcast_to(back, (rows, wide))
    for c in range(0, width, wide):
        at = slice(c, c + wide)
        grad[:, at] = (g[:, at].astype(F32) + (s * dg[:, at] - h[:, at].astype(F32) * back)).astype(BF16)


def norm_back(d, h, g, inv, gain):
    tok, width = h.shape
    blk = 48
    spec = pl.BlockSpec((blk, width), lambda i: (i, 0))
    return pl.pallas_call(
        norm_back_kernel, name="norm_back", grid=(tok // blk,),
        in_specs=[spec] * 5 + [pl.BlockSpec((blk, 128), lambda i: (i, 0)), const_spec((1, width))],
        out_specs=spec, out_shape=jax.ShapeDtypeStruct((tok, width), BF16), scratch_shapes=[pltpu.VMEM((blk, width), F32)],
        compiler_params=params(62), cost_estimate=cost(20 * tok * width, 12 * tok * width),
    )(*d, h, g, inv, gain)


def solution(mesh):
    tp_size = mesh.shape['tp']
    beside = [(i, i ^ 1) for i in range(tp_size)]
    across = [(i, i ^ 2) for i in range(tp_size)]
    diagonal = [(i, i ^ 3) for i in range(tp_size)]

    def send(x, pairs):
        return lax.ppermute(x, 'tp', pairs)

    def after(x, *others):
        return lax.optimization_barrier((x,) + others)[0]

    def step(hidden, positions, doc_ids, norm_gain, w_query, w_key, w_value, w_out, grad_out):
        batch, rows, width = hidden.shape
        tok = batch * rows
        nq, nk = w_query.shape[1], w_key.shape[1]
        group = nq // nk
        gain = norm_gain.astype(F32).reshape(1, width)

        pos1, doc1 = send(positions, beside), send(doc_ids, beside)
        pos2, doc2 = send(positions, across), send(doc_ids, across)
        h0 = hidden.reshape(tok, width)
        g0 = grad_out.reshape(tok, width)
        h2 = send(h0, across)
        h1 = send(h0, beside)
        g1 = send(g0, beside)
        g2 = send(g0, across)
        h3 = send(h2, beside)

        lane = jnp.arange(HEAD_DIM)
        inv_freq = ROPE_BASE ** (-(lane // 2 * 2).astype(F32) / HEAD_DIM)
        sign = jnp.where(lane % 2 == 0, -1.0, 1.0)

        def tables(*pos):
            angles = jnp.stack(pos).astype(F32)[..., None] * inv_freq
            return jnp.cos(angles), jnp.sin(angles) * sign

        ca, sa = [x.reshape(2 * tok, HEAD_DIM) for x in tables(positions, pos1)]
        na, inv_a, qa, ka, va = qkv(h0, h1, gain, ca, sa, w_query, w_key, w_value)
        pos2, doc2, ka = lax.optimization_barrier((pos2, doc2, ka))
        pos3, doc3 = send(pos2, beside), send(doc2, beside)
        cb, sb = [x.reshape(2 * tok, HEAD_DIM) for x in tables(pos2, pos3)]
        both = jnp.stack([jnp.concatenate([doc_ids, doc1, doc2, doc3], axis=1), jnp.concatenate([positions, pos1, pos2, pos3], axis=1)], axis=1)
        down, over = jnp.swapaxes(both, 1, 2), jnp.tile(both, (1, 1, group))
        dha = heads_grad(g0, g1, w_out, ka, cb, sb, down, over)
        nb, inv_b, qb, kb, vb, o, p0, p1, s2 = forward(
            batch, h2, h3, gain, cb, sb, w_query, w_key, w_value, qa, ka, va, down, over, w_out)
        s2 = send(s2, across)
        g3 = send(after(g2, p0), beside)
        p1 = send(p1, beside)
        dq, dk, dv, d0, d1, t2, gg = backward(
            batch, g2, g3, w_out, dha, qa, qb, ka, kb, va, vb, down, over, ca, cb, sa, sb,
            w_query, w_key, w_value, (h0, h1, h2, h3), inv_a, inv_b)
        t2, d1, gg, dq = lax.optimization_barrier((t2, d1, gg, dq))
        t2 = send(t2, across)
        d1 = send(d1, beside)
        gg1, gg2, gg3 = send(gg, beside), send(gg, across), send(gg, diagonal)
        gq, gk, gv, g_out, attn_out = weight_grads(na, nb, dq, dk, dv, o, (g0, g1, g2, g3), (p0, p1, s2), h0)
        grad_hidden = norm_back((after(d0, gk), d1, t2), h0, g0, inv_a, gain)
        grad_gain = ((gg + gg1) + (gg2 + gg3)).reshape(width)
        attn_out, grad_hidden = attn_out.reshape(hidden.shape), grad_hidden.reshape(hidden.shape)
        return (attn_out, grad_hidden, grad_gain, gq, gk, gv, g_out)

    row_spec = P('dp', 'tp', None)
    tok_spec = P('dp', 'tp')
    col_spec = P(None, 'tp')

    return jax.shard_map(
        step, mesh=mesh,
        in_specs=(row_spec, tok_spec, tok_spec, P(), col_spec, col_spec, col_spec, P('tp', None), row_spec),
        out_specs=(row_spec, row_spec, P('dp'), P('dp', 'tp'), P('dp', 'tp'), P('dp', 'tp'), P(('dp', 'tp'), None)),
        check_vma=False)
```

```python
import functools

import jax
import jax.numpy as jnp
from jax import lax
from jax.experimental import pallas as pl
from jax.experimental.pallas import tpu as pltpu
from jax.sharding import PartitionSpec as P


HEAD_DIM = 128
NORM_EPS = 1e-5
ROPE_BASE = 10000.0
LOG2_E = 1.4426950408889634
BF16 = jnp.bfloat16
F32 = jnp.float32
ANY = pl.BlockSpec(memory_space=pl.ANY)
NN = (((1,), (0,)), ((), ()))
NT = (((1,), (1,)), ((), ()))
TN = (((0,), (0,)), ((), ()))


def dot(a, b, dims=NN):
    return lax.dot_general(a, b, dims, preferred_element_type=F32)


def const_spec(shape):
    return pl.BlockSpec(shape, lambda *_: (0,) * len(shape), pipeline_mode=pl.Buffered(1))


def params(mib, *semantics):
    return pltpu.CompilerParams(dimension_semantics=semantics or ("arbitrary",), vmem_limit_bytes=mib << 20)


def cost(flops, moved):
    return pl.CostEstimate(flops=int(flops), bytes_accessed=int(moved), transcendentals=0)


def swap_pairs(x):
    lane = lax.broadcasted_iota(jnp.int32, x.shape, x.ndim - 1)
    return jnp.where(lane % 2 == 0, pltpu.roll(x, x.shape[-1] - 1, x.ndim - 1), pltpu.roll(x, 1, x.ndim - 1))


def project(step, fetch, gain, cos, sin, wq, wk, wv, n_out, inv_out, q_out, k_out, v_out, ns, ws, sem, wsem):
    tok, width = ns.shape
    nk = wk.shape[1]
    slots, _, blk = ws.shape
    q_steps = wq.shape[1] // blk
    save_n = pltpu.make_async_copy(ns, n_out, sem.at[4])
    load_kv = [pltpu.make_async_copy(w, ws.at[q_steps % slots, :, pl.ds(i * nk, nk)], sem.at[2 + i]) for i, w in enumerate((wk, wv))]

    def load_q(i):
        return pltpu.make_async_copy(wq.at[:, pl.ds(pl.multiple_of(i * blk, blk), blk)], ws.at[i % slots], wsem.at[i % slots])

    @pl.when(step == 0)
    def _():
        for c in fetch:
            c.start()
        fetch[0].wait()
        load_q(0).start()
        wide = 512

        def rows(i, _):
            at = pl.ds(pl.multiple_of(i * 48, 48), 48)
            total = jnp.zeros((48, wide), F32)
            for c in range(0, width, wide):
                x = ns[at, c:c + wide].astype(F32)
                total = total + x * x
            inv = lax.rsqrt(jnp.sum(total, axis=-1, keepdims=True) / width + NORM_EPS)
            for c in range(0, width, wide):
                x = ns[at, c:c + wide].astype(F32)
                ns[at, c:c + wide] = (x * inv * gain[:, c:c + wide]).astype(BF16)
            inv_out[at, :] = jnp.broadcast_to(inv, (48, 128))
            return 0

        chunks = tok // 48
        lax.fori_loop(0, chunks // 2, rows, 0)
        load_q(1).start()
        fetch[1].wait()
        lax.fori_loop(chunks // 2, chunks, rows, 0)
        load_q(2).start()

    @pl.when((step > 0) & (step + slots - 1 < q_steps))
    def _():
        load_q(step + slots - 1).start()

    @pl.when(step + slots - 1 == q_steps)
    def _():
        for c in load_kv:
            c.start()
        save_n.start()

    def rotated(raw):
        parts = []
        for j in range(raw.shape[1] // HEAD_DIM):
            x = raw[:, j * HEAD_DIM:(j + 1) * HEAD_DIM]
            parts.append((x * cos[...] + swap_pairs(x) * sin[...]).astype(BF16))
        return jnp.concatenate(parts, axis=1)

    @pl.when(step < q_steps)
    def _():
        load_q(step).wait()
        q_out[:, pl.ds(pl.multiple_of(step * blk, blk), blk)] = rotated(dot(ns[...], ws[step % slots]))

    @pl.when(step == q_steps)
    def _():
        for c in load_kv:
            c.wait()
        r = dot(ns[...], ws[q_steps % slots])
        k_out[...] = rotated(r[:, :nk])
        v_out[...] = r[:, nk:].astype(BF16)
        save_n.wait()


def project_out(tok, width, nq, nk):
    shapes = [jax.ShapeDtypeStruct((tok, 128), F32)] + [jax.ShapeDtypeStruct((tok, n), BF16) for n in (nq, nk, nk)]
    return [ANY] + [const_spec(x.shape) for x in shapes], [jax.ShapeDtypeStruct((tok, width), BF16)] + shapes


def project_scratch(tok, width, blk):
    return [pltpu.VMEM((tok, width), BF16), pltpu.VMEM((3, width, blk), BF16), pltpu.SemaphoreType.DMA((5,)), pltpu.SemaphoreType.DMA((3,))]


def qkv_kernel(ha, hb, *refs):
    ns, sem = refs[-4], refs[-2]
    half = ha.shape[0]
    fetch = copies_of((ha, hb), (ns.at[pl.ds(0, half)], ns.at[pl.ds(half, half)]), sem)
    project(pl.program_id(0), fetch, *refs)


def qkv(ha, hb, gain, cos, sin, wq, wk, wv):
    half, width = ha.shape
    tok = 2 * half
    nq, nk = wq.shape[1], wk.shape[1]
    blk = 2 * nk
    specs, shapes = project_out(tok, width, nq, nk)
    return pl.pallas_call(
        qkv_kernel, name="qkv", grid=(nq // blk + 1,),
        in_specs=[ANY, ANY, const_spec((1, width)), const_spec((tok, HEAD_DIM)), const_spec((tok, HEAD_DIM)), ANY, ANY, ANY],
        out_specs=specs, out_shape=shapes, scratch_shapes=project_scratch(tok, width, blk),
        compiler_params=params(62), cost_estimate=cost(2 * tok * width * (nq + 2 * nk), 2 * width * (nq + 2 * nk)),
    )(ha, hb, gain, cos, sin, wq, wk, wv)


def heads_grad_kernel(steps, ga, gb, w, *refs):
    out, gs, ws, sem, wsem = refs[-5:]
    step = pl.program_id(0)
    half = ga.shape[0]
    slots, blk = ws.shape[:2]

    def load(i):
        return pltpu.make_async_copy(w.at[pl.ds(pl.multiple_of(i * blk, blk), blk)], ws.at[i % slots], wsem.at[i % slots])

    @pl.when(step == 0)
    def _():
        loads = [pltpu.make_async_copy(ga, gs.at[pl.ds(0, half)], sem.at[0]),
                 pltpu.make_async_copy(gb, gs.at[pl.ds(half, half)], sem.at[1])]
        for c in loads:
            c.start()
        load(0).start()
        for c in loads:
            c.wait()
        for i in range(1, slots):
            load(i).start()

    @pl.when((step > 0) & (step + slots - 1 < steps))
    def _():
        load(step + slots - 1).start()

    load(step).wait()
    out[...] = dot(gs[...], ws[step % slots], NT).astype(BF16)


def heads_grad(ga, gb, w_out, *before):
    half, width = ga.shape
    tok = 2 * half
    n = w_out.shape[0]
    blk = 256
    steps = n // blk
    return pl.pallas_call(
        functools.partial(heads_grad_kernel, steps), name="heads_grad", grid=(steps,),
        in_specs=[ANY] * (3 + len(before)), out_specs=pl.BlockSpec((tok, blk), lambda i: (0, i)),
        out_shape=jax.ShapeDtypeStruct((tok, n), BF16),
        scratch_shapes=[pltpu.VMEM((tok, width), BF16), pltpu.VMEM((4, blk, width), BF16), pltpu.SemaphoreType.DMA((2,)),
                        pltpu.SemaphoreType.DMA((4,))],
        compiler_params=params(62), cost_estimate=cost(2 * tok * width * n, 2 * width * n),
    )(ga, gb, w_out, *before)


def tokens_of(refs, row, rows, batch):
    parts = []
    for ref in refs:
        for block in range(ref.shape[0] // (batch * rows)):
            parts.append(ref[pl.ds(pl.multiple_of((block * batch + row) * rows, rows), rows), :])
    return jnp.concatenate(parts, axis=0)


def put_tokens(ref, row, rows, batch, lanes, value):
    for block in range(ref.shape[0] // (batch * rows)):
        ref[pl.ds(pl.multiple_of((block * batch + row) * rows, rows), rows), lanes] = value[block * rows:(block + 1) * rows]


def heads_down(x):
    return jnp.concatenate([x[:, c:c + HEAD_DIM] for c in range(0, x.shape[1], HEAD_DIM)], axis=0)


def heads_across(x, seq):
    return jnp.concatenate([x[c:c + seq] for c in range(0, x.shape[0], seq)], axis=1)


def soft_weights(k, q, down, across):
    allowed = (down[:, 0:1] == across[0:1, :]) & (down[:, 1:2] <= across[1:2, :])
    scores = jnp.where(allowed, dot(k, q, NT), -1e30)
    e = jnp.exp2((scores - jnp.max(scores, axis=0, keepdims=True)) * (HEAD_DIM ** -0.5 * LOG2_E))
    return e, 1.0 / jnp.sum(e, axis=0, keepdims=True)


def attend_row(row, rows, batch, q_refs, k_refs, v_refs, down, across, out):
    q, k, v = (tokens_of(r, row, rows, batch) for r in (q_refs, k_refs, v_refs))
    wide = HEAD_DIM * (q.shape[1] // k.shape[1])
    for i in range(k.shape[1] // HEAD_DIM):
        at, kv = slice(i * wide, (i + 1) * wide), slice(i * HEAD_DIM, (i + 1) * HEAD_DIM)
        e, scale = soft_weights(k[:, kv], heads_down(q[:, at]), down[row], across[row])
        o = dot((e * scale).astype(BF16), v[:, kv], TN).astype(BF16)
        put_tokens(out, row, rows, batch, at, heads_across(o, k.shape[0]))


def attend_back_row(row, rows, batch, q_refs, k_refs, v_refs, g_refs, down, across, cos_refs, sin_refs, dq_out, dk_out, dv_out):
    q, k, v, g = (tokens_of(r, row, rows, batch) for r in (q_refs, k_refs, v_refs, g_refs))
    cos, sin = (tokens_of(r, row, rows, batch) * HEAD_DIM ** -0.5 for r in (cos_refs, sin_refs))
    seq = k.shape[0]
    wide = HEAD_DIM * (q.shape[1] // k.shape[1])

    def unrotated(x):
        return (x * cos - swap_pairs(x) * sin).astype(BF16)

    for i in range(k.shape[1] // HEAD_DIM):
        at, kv = slice(i * wide, (i + 1) * wide), slice(i * HEAD_DIM, (i + 1) * HEAD_DIM)
        qh, gh = heads_down(q[:, at]), heads_down(g[:, at])
        e, scale = soft_weights(k[:, kv], qh, down[row], across[row])
        probs = e * scale
        gp = dot(v[:, kv], gh, NT)
        ds = (probs * (gp - jnp.sum(probs * gp, axis=0, keepdims=True))).astype(BF16)
        put_tokens(dv_out, row, rows, batch, kv, dot(probs.astype(BF16), gh).astype(BF16))
        put_tokens(dk_out, row, rows, batch, kv, unrotated(dot(ds, qh)))
        dq = dot(ds, k[:, kv], TN)
        dq = jnp.concatenate([unrotated(dq[c:c + seq]) for c in range(0, dq.shape[0], seq)], axis=1)
        put_tokens(dq_out, row, rows, batch, at, dq)


def other_core():
    tp = lax.axis_index("tp")
    return {"tp": tp + 1 - 2 * lax.rem(tp, 2)}


def greet():
    @pl.when(pl.program_id(0) == 0)
    def _():
        barrier = pltpu.get_barrier_semaphore()
        pl.semaphore_signal(barrier, inc=1, device_id=other_core(), device_id_type=pl.DeviceIdType.MESH)
        pl.semaphore_wait(barrier, 1)


def chip_sum(first, steps, share, out, keep, box, got, send_sem, recv_sem):
    step = pl.program_id(0) - first
    neighbour = other_core()

    def copy(i):
        return pltpu.make_async_remote_copy(box.at[i % 2], got.at[i % 2], send_sem.at[i % 2], recv_sem.at[i % 2],
                                            device_id=neighbour, device_id_type=pl.DeviceIdType.MESH)

    @pl.when(step > 0)
    def _():
        copy(step - 1).start()

    @pl.when((step >= 0) & (step < steps))
    def _():
        counterpart, diagonal = share()
        keep[step % 2] = counterpart
        box[step % 2] = diagonal

    @pl.when(step > 0)
    def _():
        copy(step - 1).wait()
        out[...] = (keep[(step - 1) % 2] + got[(step - 1) % 2]).astype(BF16)


def chip_sum_scratch(rows, blk):
    return [pltpu.VMEM((2, rows, blk), F32)] * 3 + [pltpu.SemaphoreType.DMA((2,))] * 2


def start_all(copies):
    for c in copies:
        c.start()


def wait_all(copies):
    for c in copies:
        c.wait()


def copies_of(sources, targets, sem):
    return [pltpu.make_async_copy(a, b, sem.at[i]) for i, (a, b) in enumerate(zip(sources, targets))]


def like(*arrays):
    return [pltpu.VMEM(x.shape, x.dtype) for x in arrays]


def clip(i, n):
    return jnp.clip(i, 0, n - 1)


def comm_params(number):
    return pltpu.CompilerParams(dimension_semantics=("arbitrary",), vmem_limit_bytes=62 << 20, collective_id=number, has_side_effects=True)


def forward_kernel(batch, first, steps, h2, gain, cos, sin, wq, wk, wv, qa_in, ka_in, va_in, down, across, w_out,
                   n_out, inv_out, qb_out, kb_out, vb_out, o_out, h3, p0, p1, s2,
                   ns, ws, sem, wsem, wo, osem, qa, ka, va, qb, kb, vb, o, isem, esem, xsem, *chip):
    step = pl.program_id(0)
    slots, _, blk = wo.shape
    attend_at = first - batch
    loads = copies_of((qa_in, ka_in, va_in), (qa, ka, va), isem)
    saves = copies_of((qb, kb, vb, o), (qb_out, kb_out, vb_out, o_out), esem)

    half = h2.shape[0]
    fetch = [pltpu.make_async_copy(h2, ns.at[pl.ds(0, half)], sem.at[0])] + [
        pltpu.make_async_remote_copy(h2, to, xsem.at[0, i], xsem.at[1, i], device_id=other_core(), device_id_type=pl.DeviceIdType.MESH)
        for i, to in enumerate((ns.at[pl.ds(half, half)], h3))]
    greet()

    @pl.when(step == 1)
    def _():
        start_all(loads)
        fetch[2].start()

    def load(i):
        return pltpu.make_async_copy(w_out.at[:, pl.ds(pl.multiple_of(i * blk, blk), blk)], wo.at[i % slots], osem.at[i % slots])

    @pl.when(step < attend_at)
    def _():
        project(step, fetch[:2], gain, cos, sin, wq, wk, wv, n_out, inv_out, qb, kb, vb, ns, ws, sem, wsem)

    @pl.when(step == attend_at - 1)
    def _():
        for i in range(slots):
            load(i).start()

    @pl.when(step == attend_at)
    def _():
        wait_all(loads)
        start_all(saves[:3])

    @pl.when(step == first)
    def _():
        saves[3].start()

    @pl.when((step >= attend_at) & (step < first))
    def _():
        rows = qa.shape[0] // (2 * batch)
        attend_row(step - attend_at, rows, batch, (qa, qb), (ka, kb), (va, vb), down, across, o)

    @pl.when((step > first) & (step - first + slots - 1 < steps))
    def _():
        load(step - first + slots - 1).start()

    def share():
        load(step - first).wait()
        r = dot(o[...], wo[(step - first) % slots])
        rows = p0.shape[0]
        p0[...] = r[:rows].astype(BF16)
        p1[...] = r[rows:2 * rows].astype(BF16)
        return r[2 * rows:3 * rows], r[3 * rows:]

    chip_sum(first, steps, share, s2, *chip)

    @pl.when(step == first + steps)
    def _():
        wait_all(saves)
        fetch[2].wait()


def forward(batch, h2, gain, cos, sin, wq, wk, wv, qa, ka, va, down, across, w_out):
    half, width = h2.shape
    tok = 2 * half
    nq, nk = wq.shape[1], wk.shape[1]
    wide, blk = 2 * nk, 1024
    first, steps = nq // wide + 1 + batch, width // blk
    specs, shapes = project_out(tok, width, nq, nk)
    now = pl.BlockSpec((half, blk), lambda i: (0, clip(i - first, steps)))
    late = pl.BlockSpec((half, blk), lambda i: (0, clip(i - first - 1, steps)))
    return pl.pallas_call(
        functools.partial(forward_kernel, batch, first, steps), name="forward", grid=(first + steps + 1,),
        in_specs=[ANY] + [const_spec(x.shape) for x in (gain, cos, sin)] + [ANY] * 3
        + [ANY] * 3 + [const_spec(x.shape) for x in (down, across)] + [ANY],
        out_specs=specs[:2] + [ANY] * 5 + [now, now, late],
        out_shape=shapes + [jax.ShapeDtypeStruct((2 * tok, nq), BF16)] + [jax.ShapeDtypeStruct((half, width), BF16)] * 4,
        scratch_shapes=project_scratch(tok, width, wide) + [pltpu.VMEM((3, nq, blk), BF16), pltpu.SemaphoreType.DMA((3,))]
        + like(qa, ka, va, qa, ka, va) + [pltpu.VMEM((2 * tok, nq), BF16), pltpu.SemaphoreType.DMA((3,)), pltpu.SemaphoreType.DMA((4,)), pltpu.SemaphoreType.DMA((2, 2))]
        + chip_sum_scratch(half, blk),
        compiler_params=comm_params(0), cost_estimate=cost(2 * tok * width * (3 * nq + 2 * nk), 4 * width * nq),
    )(h2, gain, cos, sin, wq, wk, wv, qa, ka, va, down, across, w_out)


def backward_kernel(batch, heads_steps, steps, ga, gb, w_out, down, across, wq, wk, wv, h0, h1, h2, h3, inv_a, inv_b, *refs):
    kept_in, (dq_out, dk_out, dv_out, d0, d1, t2, gain), kept = refs[:11], refs[11:18], refs[18:29]
    gh_a, qa, qb, ka, kb, va, vb, ca, cb, sa, sb = kept
    grads, gs, gh_b, wo, ws, sem, osem, wsem, isem, esem = refs[29:39]
    chip = refs[39:]
    step = pl.program_id(0)
    loads = copies_of(kept_in, kept, isem)
    nq, nk = wq.shape[1], wk.shape[1]
    lanes = [pl.ds(0, nq), pl.ds(nq, nk), pl.ds(nq + nk, nk)]
    dq, dk, dv = [grads.at[:, at] for at in lanes]
    saves = copies_of((dq, dk, dv), (dq_out, dk_out, dv_out), esem)
    greet()
    half = ga.shape[0]
    slots, blk = wo.shape[:2]
    w_slots, wide = ws.shape[:2]
    first = heads_steps + batch

    def load(i):
        return pltpu.make_async_copy(w_out.at[pl.ds(pl.multiple_of(i * blk, blk), blk)], wo.at[i % slots], osem.at[i % slots])

    def load_w(i):
        at = pl.ds(pl.multiple_of(i * wide, wide), wide)
        return [pltpu.make_async_copy(w.at[at], ws.at[i % w_slots, :, lanes[j]], wsem.at[j, i % w_slots]) for j, w in enumerate((wq, wk, wv))]

    def start_w(i):
        for c in load_w(i):
            c.start()

    @pl.when(step == 0)
    def _():
        fetch = copies_of((ga, gb), (gs.at[pl.ds(0, half)], gs.at[pl.ds(half, half)]), sem)
        start_all(fetch)
        load(0).start()
        wait_all(fetch)
        for i in range(1, slots):
            load(i).start()

    @pl.when(step == heads_steps // 2)
    def _():
        start_all(loads)

    @pl.when(step == heads_steps)
    def _():
        wait_all(loads)

    @pl.when(step == first)
    def _():
        start_all(saves)

    @pl.when((step > 0) & (step + slots - 1 < heads_steps))
    def _():
        load(step + slots - 1).start()

    @pl.when(step < heads_steps)
    def _():
        load(step).wait()
        gh_b[:, pl.ds(pl.multiple_of(step * blk, blk), blk)] = dot(gs[...], wo[step % slots], NT).astype(BF16)

    @pl.when(step == heads_steps - 1)
    def _():
        for i in range(w_slots):
            start_w(i)

    @pl.when((step >= heads_steps) & (step < first))
    def _():
        rows = qa.shape[0] // (2 * batch)
        attend_back_row(step - heads_steps, rows, batch, (qa, qb), (ka, kb), (va, vb), (gh_a, gh_b), down, across, (ca, cb), (sa, sb), dq, dk, dv)

    @pl.when((step > first) & (step - first + w_slots - 1 < steps))
    def _():
        start_w(step - first + w_slots - 1)

    def share():
        i = step - first
        for c in load_w(i):
            c.wait()
        r = dot(grads[...], ws[i % w_slots], NT)
        parts = [r[j * half:(j + 1) * half] for j in range(4)]
        d0[...] = parts[0].astype(BF16)
        d1[...] = parts[1].astype(BF16)
        total = 0.0
        for j, (part, h) in enumerate(zip(parts, (h0, h1, h2, h3))):
            inv = (inv_a, inv_b)[j // 2][(j % 2) * half:(j % 2 + 1) * half, :1]
            total = total + jnp.sum(part * (h[...].astype(F32) * inv), axis=0, keepdims=True)
        gain[...] = total
        return parts[2], parts[3]

    chip_sum(first, steps, share, t2, *chip)

    @pl.when(step == first + steps)
    def _():
        wait_all(saves)


def backward(batch, ga, gb, w_out, gh_a, qa, qb, ka, kb, va, vb, down, across, ca, cb, sa, sb, wq, wk, wv, h, inv_a, inv_b):
    half, width = ga.shape
    tok = 4 * half
    nq, nk = wq.shape[1], wk.shape[1]
    blk, wide = 256, 1024
    heads_steps, steps = nq // blk, width // wide
    first = heads_steps + batch
    now = pl.BlockSpec((half, wide), lambda i: (0, clip(i - first, steps)))
    late = pl.BlockSpec((half, wide), lambda i: (0, clip(i - first - 1, steps)))
    kept = (gh_a, qa, qb, ka, kb, va, vb, ca, cb, sa, sb)
    return pl.pallas_call(
        functools.partial(backward_kernel, batch, heads_steps, steps), name="backward", grid=(first + steps + 1,),
        in_specs=[ANY] * 3 + [const_spec(x.shape) for x in (down, across)] + [ANY] * 3 + [now] * 4
        + [const_spec(x.shape) for x in (inv_a, inv_b)] + [ANY] * len(kept),
        out_specs=[ANY] * 3 + [now, now, late, pl.BlockSpec((1, wide), lambda i: (0, clip(i - first, steps)))],
        out_shape=[jax.ShapeDtypeStruct((tok, n), BF16) for n in (nq, nk, nk)] + [jax.ShapeDtypeStruct((half, width), BF16)] * 3
        + [jax.ShapeDtypeStruct((1, width), F32)],
        scratch_shapes=like(*kept) + [pltpu.VMEM((tok, nq + 2 * nk), BF16)]
        + [pltpu.VMEM((2 * half, width), BF16), pltpu.VMEM((2 * half, nq), BF16), pltpu.VMEM((4, blk, width), BF16),
           pltpu.VMEM((3, wide, nq + 2 * nk), BF16),
           pltpu.SemaphoreType.DMA((2,)), pltpu.SemaphoreType.DMA((4,)), pltpu.SemaphoreType.DMA((3, 3)),
           pltpu.SemaphoreType.DMA((len(kept),)), pltpu.SemaphoreType.DMA((3,))]
        + chip_sum_scratch(half, wide),
        compiler_params=comm_params(1), cost_estimate=cost(2 * tok * width * (2 * nq + 2 * nk), 4 * width * nq),
    )(ga, gb, w_out, down, across, wq, wk, wv, *h, inv_a, inv_b, *kept)


def weight_grads_kernel(steps, na, nb, dq, dk, dv, o_in, g0, g1, g2, g3, p0, p1, p2, h, gq, gk, gv, g_out, out, o, ot, sem):
    step = pl.program_id(0)
    load = pltpu.make_async_copy(o_in, o, sem)

    @pl.when(step == 1)
    def _():
        load.start()

    @pl.when(step < steps)
    def _():
        n = jnp.concatenate([na[...], nb[...]], axis=0).T
        for d, grad in ((dq, gq), (dk, gk), (dv, gv)):
            grad[...] = dot(n, d[...])

    @pl.when(step == steps)
    def _():
        load.wait()
        for c in range(0, o.shape[1], 256):
            ot[c:c + 256, :] = o[:, c:c + 256].T

    @pl.when(step >= steps)
    def _():
        g_out[...] = dot(ot[...], jnp.concatenate([g0[...], g1[...], g2[...], g3[...]], axis=0))
        share = sum(x[...].astype(F32) for x in (p0, p1, p2))
        out[...] = (h[...].astype(F32) + share.astype(BF16).astype(F32)).astype(BF16)


def weight_grads(na, nb, dq, dk, dv, o, g, p, h):
    tok, nq = dq.shape
    nk = dk.shape[1]
    width = na.shape[1]
    blk = 1024
    steps = width // blk

    def early(i):
        return jnp.minimum(i, steps - 1)

    def late(i):
        return jnp.maximum(i - steps, 0)

    rows = pl.BlockSpec((tok // 4, blk), lambda i: (0, late(i)))
    return pl.pallas_call(
        functools.partial(weight_grads_kernel, steps), name="weight_grads", grid=(2 * steps,),
        in_specs=[pl.BlockSpec((tok // 2, blk), lambda i: (0, early(i)))] * 2 + [const_spec((tok, nq))] + [const_spec((tok, nk))] * 2
        + [ANY] + [rows] * 8,
        out_specs=[pl.BlockSpec((blk, n), lambda i: (early(i), 0)) for n in (nq, nk, nk)] + [pl.BlockSpec((nq, blk), lambda i: (0, late(i))), rows],
        out_shape=[jax.ShapeDtypeStruct((width, n), F32) for n in (nq, nk, nk)]
        + [jax.ShapeDtypeStruct((nq, width), F32), jax.ShapeDtypeStruct(h.shape, BF16)],
        scratch_shapes=[pltpu.VMEM((tok, nq), BF16), pltpu.VMEM((nq, tok), BF16), pltpu.SemaphoreType.DMA],
        compiler_params=params(62), cost_estimate=cost(4 * tok * width * (nq + nk), 8 * width * (nq + nk)),
    )(na, nb, dq, dk, dv, o, *g, *p, h)


def norm_back_kernel(d0, d1, d2, h, g, inv, gain, gg0, gg1, gg2, gg3, grad, grad_gain, *refs):
    held, (out, dg, isem, esem) = refs[:5], refs[5:]
    rows, width = dg.shape
    count = out.shape[0] // rows
    wide = 1024

    def at(i):
        return pl.ds(pl.multiple_of(i * rows, rows), rows)

    def loads(i):
        return [pltpu.make_async_copy(a.at[at(i)], b.at[at(i)], isem.at[j, i]) for j, (a, b) in enumerate(zip((d0, d1, d2, h, g), held))]

    def save(i):
        return pltpu.make_async_copy(out.at[at(i)], grad.at[at(i)], esem.at[i])

    @pl.loop(0, count)
    def _(i):
        start_all(loads(i))

    grad_gain[...] = (gg0[...] + gg1[...]) + (gg2[...] + gg3[...])
    x0, x1, x2, hs, gs = held

    @pl.loop(0, count)
    def _(i):
        wait_all(loads(i))
        total = jnp.zeros((rows, wide), F32)
        for c in range(0, width, wide):
            cut = slice(c, c + wide)
            x = sum(d[at(i), cut].astype(F32) for d in (x0, x1, x2)) * gain[:, cut]
            dg[:, cut] = x
            total = total + x * hs[at(i), cut].astype(F32)
        s = inv[at(i), :1]
        back = (s * s * s) * (jnp.sum(total, axis=-1, keepdims=True) / width)
        s = jnp.broadcast_to(s, (rows, wide))
        back = jnp.broadcast_to(back, (rows, wide))
        for c in range(0, width, wide):
            cut = slice(c, c + wide)
            out[at(i), cut] = (gs[at(i), cut].astype(F32) + (s * dg[:, cut] - hs[at(i), cut].astype(F32) * back)).astype(BF16)
        save(i).start()

    @pl.loop(0, count)
    def _(i):
        save(i).wait()


def norm_back(d, h, g, inv, gain, gain_shares):
    tok, width = h.shape
    rows = 16
    count = tok // rows
    whole = pl.BlockSpec(memory_space=pltpu.VMEM)
    return pl.pallas_call(
        norm_back_kernel, name="norm_back", in_specs=[ANY] * 5 + [whole] * 6, out_specs=[ANY, whole],
        out_shape=[jax.ShapeDtypeStruct((tok, width), BF16), jax.ShapeDtypeStruct((1, width), F32)],
        scratch_shapes=[pltpu.VMEM((tok, width), BF16)] * 6
        + [pltpu.VMEM((rows, width), F32), pltpu.SemaphoreType.DMA((5, count)), pltpu.SemaphoreType.DMA((count,))],
        compiler_params=pltpu.CompilerParams(vmem_limit_bytes=62 << 20), cost_estimate=cost(20 * tok * width, 12 * tok * width),
    )(*d, h, g, inv, gain, *gain_shares)


def solution(mesh):
    tp_size = mesh.shape['tp']
    beside = [(i, i ^ 1) for i in range(tp_size)]
    across = [(i, i ^ 2) for i in range(tp_size)]
    diagonal = [(i, i ^ 3) for i in range(tp_size)]

    def send(x, pairs):
        return lax.ppermute(x, 'tp', pairs)

    def after(x, *others):
        return lax.optimization_barrier((x,) + others)[0]

    def step(hidden, positions, doc_ids, norm_gain, w_query, w_key, w_value, w_out, grad_out):
        batch, rows, width = hidden.shape
        tok = batch * rows
        nq, nk = w_query.shape[1], w_key.shape[1]
        group = nq // nk
        gain = norm_gain.astype(F32).reshape(1, width)

        pos1, doc1 = send(positions, beside), send(doc_ids, beside)
        pos2, doc2 = send(positions, across), send(doc_ids, across)
        h0 = hidden.reshape(tok, width)
        g0 = grad_out.reshape(tok, width)
        h2 = send(h0, across)
        h1 = send(h0, beside)
        g1 = send(g0, beside)
        g2 = send(g0, across)

        lane = jnp.arange(HEAD_DIM)
        inv_freq = ROPE_BASE ** (-(lane // 2 * 2).astype(F32) / HEAD_DIM)
        sign = jnp.where(lane % 2 == 0, -1.0, 1.0)

        def tables(*pos):
            angles = jnp.stack(pos).astype(F32)[..., None] * inv_freq
            return jnp.cos(angles), jnp.sin(angles) * sign

        ca, sa = [x.reshape(2 * tok, HEAD_DIM) for x in tables(positions, pos1)]
        na, inv_a, qa, ka, va = qkv(h0, h1, gain, ca, sa, w_query, w_key, w_value)
        pos2, doc2, ka = lax.optimization_barrier((pos2, doc2, ka))
        pos3, doc3 = send(pos2, beside), send(doc2, beside)
        cb, sb = [x.reshape(2 * tok, HEAD_DIM) for x in tables(pos2, pos3)]
        both = jnp.stack([jnp.concatenate([doc_ids, doc1, doc2, doc3], axis=1), jnp.concatenate([positions, pos1, pos2, pos3], axis=1)], axis=1)
        down, over = jnp.swapaxes(both, 1, 2), jnp.tile(both, (1, 1, group))
        dha = heads_grad(g0, g1, w_out, ka, cb, sb, down, over)
        nb, inv_b, qb, kb, vb, o, h3, p0, p1, s2 = forward(
            batch, h2, gain, cb, sb, w_query, w_key, w_value, qa, ka, va, down, over, w_out)
        s2 = send(s2, across)
        g3 = send(after(g2, p0), beside)
        p1 = send(p1, beside)
        dq, dk, dv, d0, d1, t2, gg = backward(
            batch, g2, g3, w_out, dha, qa, qb, ka, kb, va, vb, down, over, ca, cb, sa, sb,
            w_query, w_key, w_value, (h0, h1, h2, h3), inv_a, inv_b)
        t2, d1, gg, dq = lax.optimization_barrier((t2, d1, gg, dq))
        t2 = send(t2, across)
        d1 = send(d1, beside)
        gg1, gg2, gg3 = send(gg, beside), send(gg, across), send(gg, diagonal)
        gq, gk, gv, g_out, attn_out = weight_grads(na, nb, dq, dk, dv, o, (g0, g1, g2, g3), (p0, p1, s2), h0)
        grad_hidden, gg = norm_back((after(d0, gk), d1, t2), h0, g0, inv_a[:tok], gain, (gg, gg1, gg2, gg3))
        grad_gain = gg.reshape(width)
        attn_out, grad_hidden = attn_out.reshape(hidden.shape), grad_hidden.reshape(hidden.shape)
        return (attn_out, grad_hidden, grad_gain, gq, gk, gv, g_out)

    row_spec = P('dp', 'tp', None)
    tok_spec = P('dp', 'tp')
    col_spec = P(None, 'tp')

    return jax.shard_map(
        step, mesh=mesh,
        in_specs=(row_spec, tok_spec, tok_spec, P(), col_spec, col_spec, col_spec, P('tp', None), row_spec),
        out_specs=(row_spec, row_spec, P('dp'), P('dp', 'tp'), P('dp', 'tp'), P('dp', 'tp'), P(('dp', 'tp'), None)),
        check_vma=False)
```

```python
import functools

import jax
import jax.numpy as jnp
from jax import lax
from jax.experimental import pallas as pl
from jax.experimental.pallas import tpu as pltpu
from jax.sharding import PartitionSpec as P


HEAD_DIM = 128
NORM_EPS = 1e-5
ROPE_BASE = 10000.0
LOG2_E = 1.4426950408889634
BF16 = jnp.bfloat16
F32 = jnp.float32
ANY = pl.BlockSpec(memory_space=pl.ANY)
NN = (((1,), (0,)), ((), ()))
NT = (((1,), (1,)), ((), ()))
TN = (((0,), (0,)), ((), ()))


def dot(a, b, dims=NN):
    return lax.dot_general(a, b, dims, preferred_element_type=F32)


def const_spec(shape):
    return pl.BlockSpec(shape, lambda *_: (0,) * len(shape), pipeline_mode=pl.Buffered(1))


def params(mib, *semantics):
    return pltpu.CompilerParams(dimension_semantics=semantics or ("arbitrary",), vmem_limit_bytes=mib << 20)


def cost(flops, moved):
    return pl.CostEstimate(flops=int(flops), bytes_accessed=int(moved), transcendentals=0)


def swap_pairs(x):
    lane = lax.broadcasted_iota(jnp.int32, x.shape, x.ndim - 1)
    return jnp.where(lane % 2 == 0, pltpu.roll(x, x.shape[-1] - 1, x.ndim - 1), pltpu.roll(x, 1, x.ndim - 1))


def project(step, fetch, gain, cos, sin, wq, wk, wv, n_out, inv_out, q_out, k_out, v_out, ns, ws, sem, wsem):
    tok, width = ns.shape
    nk = wk.shape[1]
    slots, _, blk = ws.shape
    q_steps = wq.shape[1] // blk
    save_n = pltpu.make_async_copy(ns, n_out, sem.at[4])
    load_kv = [pltpu.make_async_copy(w, ws.at[q_steps % slots, :, pl.ds(i * nk, nk)], sem.at[2 + i]) for i, w in enumerate((wk, wv))]

    def load_q(i):
        return pltpu.make_async_copy(wq.at[:, pl.ds(pl.multiple_of(i * blk, blk), blk)], ws.at[i % slots], wsem.at[i % slots])

    @pl.when(step == 0)
    def _():
        for c in fetch:
            c.start()
        fetch[0].wait()
        load_q(0).start()
        wide = 512

        def rows(i, _):
            at = pl.ds(pl.multiple_of(i * 48, 48), 48)
            total = jnp.zeros((48, wide), F32)
            for c in range(0, width, wide):
                x = ns[at, c:c + wide].astype(F32)
                total = total + x * x
            inv = lax.rsqrt(jnp.sum(total, axis=-1, keepdims=True) / width + NORM_EPS)
            for c in range(0, width, wide):
                x = ns[at, c:c + wide].astype(F32)
                ns[at, c:c + wide] = (x * inv * gain[:, c:c + wide]).astype(BF16)
            inv_out[at, :] = jnp.broadcast_to(inv, (48, 128))
            return 0

        chunks = tok // 48
        lax.fori_loop(0, chunks // 2, rows, 0)
        load_q(1).start()
        fetch[1].wait()
        lax.fori_loop(chunks // 2, chunks, rows, 0)
        load_q(2).start()

    @pl.when((step > 0) & (step + slots - 1 < q_steps))
    def _():
        load_q(step + slots - 1).start()

    @pl.when(step + slots - 1 == q_steps)
    def _():
        for c in load_kv:
            c.start()
        save_n.start()

    def rotated(raw):
        parts = []
        for j in range(raw.shape[1] // HEAD_DIM):
            x = raw[:, j * HEAD_DIM:(j + 1) * HEAD_DIM]
            parts.append((x * cos[...] + swap_pairs(x) * sin[...]).astype(BF16))
        return jnp.concatenate(parts, axis=1)

    @pl.when(step < q_steps)
    def _():
        load_q(step).wait()
        q_out[:, pl.ds(pl.multiple_of(step * blk, blk), blk)] = rotated(dot(ns[...], ws[step % slots]))

    @pl.when(step == q_steps)
    def _():
        for c in load_kv:
            c.wait()
        r = dot(ns[...], ws[q_steps % slots])
        k_out[...] = rotated(r[:, :nk])
        v_out[...] = r[:, nk:].astype(BF16)
        save_n.wait()


def project_out(tok, width, nq, nk):
    shapes = [jax.ShapeDtypeStruct((tok, 128), F32)] + [jax.ShapeDtypeStruct((tok, n), BF16) for n in (nq, nk, nk)]
    return [ANY] + [const_spec(x.shape) for x in shapes], [jax.ShapeDtypeStruct((tok, width), BF16)] + shapes


def project_scratch(tok, width, blk):
    return [pltpu.VMEM((tok, width), BF16), pltpu.VMEM((3, width, blk), BF16), pltpu.SemaphoreType.DMA((5,)), pltpu.SemaphoreType.DMA((3,))]


def qkv_kernel(ha, hb, *refs):
    ns, sem = refs[-4], refs[-2]
    half = ha.shape[0]
    fetch = copies_of((ha, hb), (ns.at[pl.ds(0, half)], ns.at[pl.ds(half, half)]), sem)
    project(pl.program_id(0), fetch, *refs)


def qkv(ha, hb, gain, cos, sin, wq, wk, wv):
    half, width = ha.shape
    tok = 2 * half
    nq, nk = wq.shape[1], wk.shape[1]
    blk = 2 * nk
    specs, shapes = project_out(tok, width, nq, nk)
    return pl.pallas_call(
        qkv_kernel, name="qkv", grid=(nq // blk + 1,),
        in_specs=[ANY, ANY, const_spec((1, width)), const_spec((tok, HEAD_DIM)), const_spec((tok, HEAD_DIM)), ANY, ANY, ANY],
        out_specs=specs, out_shape=shapes, scratch_shapes=project_scratch(tok, width, blk),
        compiler_params=params(62), cost_estimate=cost(2 * tok * width * (nq + 2 * nk), 2 * width * (nq + 2 * nk)),
    )(ha, hb, gain, cos, sin, wq, wk, wv)


def heads_grad_kernel(steps, ga, gb, w, *refs):
    out, gs, ws, sem, wsem = refs[-5:]
    step = pl.program_id(0)
    half = ga.shape[0]
    slots, blk = ws.shape[:2]

    def load(i):
        return pltpu.make_async_copy(w.at[pl.ds(pl.multiple_of(i * blk, blk), blk)], ws.at[i % slots], wsem.at[i % slots])

    @pl.when(step == 0)
    def _():
        loads = [pltpu.make_async_copy(ga, gs.at[pl.ds(0, half)], sem.at[0]),
                 pltpu.make_async_copy(gb, gs.at[pl.ds(half, half)], sem.at[1])]
        for c in loads:
            c.start()
        load(0).start()
        for c in loads:
            c.wait()
        for i in range(1, slots):
            load(i).start()

    @pl.when((step > 0) & (step + slots - 1 < steps))
    def _():
        load(step + slots - 1).start()

    load(step).wait()
    out[...] = dot(gs[...], ws[step % slots], NT).astype(BF16)


def heads_grad(ga, gb, w_out, *before):
    half, width = ga.shape
    tok = 2 * half
    n = w_out.shape[0]
    blk = 256
    steps = n // blk
    return pl.pallas_call(
        functools.partial(heads_grad_kernel, steps), name="heads_grad", grid=(steps,),
        in_specs=[ANY] * (3 + len(before)), out_specs=pl.BlockSpec((tok, blk), lambda i: (0, i)),
        out_shape=jax.ShapeDtypeStruct((tok, n), BF16),
        scratch_shapes=[pltpu.VMEM((tok, width), BF16), pltpu.VMEM((4, blk, width), BF16), pltpu.SemaphoreType.DMA((2,)),
                        pltpu.SemaphoreType.DMA((4,))],
        compiler_params=params(62), cost_estimate=cost(2 * tok * width * n, 2 * width * n),
    )(ga, gb, w_out, *before)


def tokens_of(refs, row, rows, batch):
    parts = []
    for ref in refs:
        for block in range(ref.shape[0] // (batch * rows)):
            parts.append(ref[pl.ds(pl.multiple_of((block * batch + row) * rows, rows), rows), :])
    return jnp.concatenate(parts, axis=0)


def put_tokens(ref, row, rows, batch, lanes, value):
    for block in range(ref.shape[0] // (batch * rows)):
        ref[pl.ds(pl.multiple_of((block * batch + row) * rows, rows), rows), lanes] = value[block * rows:(block + 1) * rows]


def heads_down(x):
    return jnp.concatenate([x[:, c:c + HEAD_DIM] for c in range(0, x.shape[1], HEAD_DIM)], axis=0)


def heads_across(x, seq):
    return jnp.concatenate([x[c:c + seq] for c in range(0, x.shape[0], seq)], axis=1)


def soft_weights(k, q, down, across):
    allowed = (down[:, 0:1] == across[0:1, :]) & (down[:, 1:2] <= across[1:2, :])
    scores = jnp.where(allowed, dot(k, q, NT), -1e30)
    e = jnp.exp2((scores - jnp.max(scores, axis=0, keepdims=True)) * (HEAD_DIM ** -0.5 * LOG2_E))
    return e, 1.0 / jnp.sum(e, axis=0, keepdims=True)


def attend_row(row, rows, batch, q_refs, k_refs, v_refs, down, across, out):
    q, k, v = (tokens_of(r, row, rows, batch) for r in (q_refs, k_refs, v_refs))
    wide = HEAD_DIM * (q.shape[1] // k.shape[1])
    for i in range(k.shape[1] // HEAD_DIM):
        at, kv = slice(i * wide, (i + 1) * wide), slice(i * HEAD_DIM, (i + 1) * HEAD_DIM)
        e, scale = soft_weights(k[:, kv], heads_down(q[:, at]), down[row], across[row])
        o = dot((e * scale).astype(BF16), v[:, kv], TN).astype(BF16)
        put_tokens(out, row, rows, batch, at, heads_across(o, k.shape[0]))


def attend_back_row(row, rows, batch, q_refs, k_refs, v_refs, g_refs, down, across, cos_refs, sin_refs, dq_out, dk_out, dv_out):
    q, k, v, g = (tokens_of(r, row, rows, batch) for r in (q_refs, k_refs, v_refs, g_refs))
    cos, sin = (tokens_of(r, row, rows, batch) * HEAD_DIM ** -0.5 for r in (cos_refs, sin_refs))
    seq = k.shape[0]
    wide = HEAD_DIM * (q.shape[1] // k.shape[1])

    def unrotated(x):
        return (x * cos - swap_pairs(x) * sin).astype(BF16)

    for i in range(k.shape[1] // HEAD_DIM):
        at, kv = slice(i * wide, (i + 1) * wide), slice(i * HEAD_DIM, (i + 1) * HEAD_DIM)
        qh, gh = heads_down(q[:, at]), heads_down(g[:, at])
        e, scale = soft_weights(k[:, kv], qh, down[row], across[row])
        probs = e * scale
        gp = dot(v[:, kv], gh, NT)
        ds = (probs * (gp - jnp.sum(probs * gp, axis=0, keepdims=True))).astype(BF16)
        put_tokens(dv_out, row, rows, batch, kv, dot(probs.astype(BF16), gh).astype(BF16))
        put_tokens(dk_out, row, rows, batch, kv, unrotated(dot(ds, qh)))
        dq = dot(ds, k[:, kv], TN)
        dq = jnp.concatenate([unrotated(dq[c:c + seq]) for c in range(0, dq.shape[0], seq)], axis=1)
        put_tokens(dq_out, row, rows, batch, at, dq)


def other_core():
    tp = lax.axis_index("tp")
    return {"tp": tp + 1 - 2 * lax.rem(tp, 2)}


def greet():
    @pl.when(pl.program_id(0) == 0)
    def _():
        barrier = pltpu.get_barrier_semaphore()
        pl.semaphore_signal(barrier, inc=1, device_id=other_core(), device_id_type=pl.DeviceIdType.MESH)
        pl.semaphore_wait(barrier, 1)


def chip_sum(first, steps, share, outs, keep, box, got, send_sem, recv_sem):
    step = pl.program_id(0) - first
    neighbour = other_core()

    def copy(i):
        return pltpu.make_async_remote_copy(box.at[i % 2], got.at[i % 2], send_sem.at[i % 2], recv_sem.at[i % 2],
                                            device_id=neighbour, device_id_type=pl.DeviceIdType.MESH)

    @pl.when(step > 0)
    def _():
        copy(step - 1).start()

    @pl.when((step >= 0) & (step < steps))
    def _():
        at = 0
        for mine, theirs in share():
            keep[step % 2, at:at + mine.shape[0]] = mine
            box[step % 2, at:at + mine.shape[0]] = theirs
            at += mine.shape[0]

    @pl.when(step > 0)
    def _():
        copy(step - 1).wait()
        at = 0
        for out in outs:
            cut = slice(at, at + out.shape[0])
            out[...] = (keep[(step - 1) % 2, cut] + got[(step - 1) % 2, cut]).astype(out.dtype)
            at += out.shape[0]


def chip_sum_scratch(rows, blk):
    return [pltpu.VMEM((2, rows, blk), F32)] * 3 + [pltpu.SemaphoreType.DMA((2,))] * 2


def start_all(copies):
    for c in copies:
        c.start()


def wait_all(copies):
    for c in copies:
        c.wait()


def copies_of(sources, targets, sem):
    return [pltpu.make_async_copy(a, b, sem.at[i]) for i, (a, b) in enumerate(zip(sources, targets))]


def like(*arrays):
    return [pltpu.VMEM(x.shape, x.dtype) for x in arrays]


def clip(i, n):
    return jnp.clip(i, 0, n - 1)


def comm_params(number):
    return pltpu.CompilerParams(dimension_semantics=("arbitrary",), vmem_limit_bytes=62 << 20, collective_id=number, has_side_effects=True)


def forward_kernel(batch, first, steps, h2, gain, cos, sin, wq, wk, wv, qa_in, ka_in, va_in, down, across, w_out,
                   n_out, inv_out, qb_out, kb_out, vb_out, o_out, h3, p0, p1, s2,
                   ns, ws, sem, wsem, wo, osem, qa, ka, va, qb, kb, vb, o, isem, esem, xsem, *chip):
    step = pl.program_id(0)
    slots, _, blk = wo.shape
    attend_at = first - batch
    loads = copies_of((qa_in, ka_in, va_in), (qa, ka, va), isem)
    saves = copies_of((qb, kb, vb, o), (qb_out, kb_out, vb_out, o_out), esem)

    half = h2.shape[0]
    fetch = [pltpu.make_async_copy(h2, ns.at[pl.ds(0, half)], sem.at[0])] + [
        pltpu.make_async_remote_copy(h2, to, xsem.at[0, i], xsem.at[1, i], device_id=other_core(), device_id_type=pl.DeviceIdType.MESH)
        for i, to in enumerate((ns.at[pl.ds(half, half)], h3))]
    greet()

    @pl.when(step == 1)
    def _():
        start_all(loads)
        fetch[2].start()

    def load(i):
        return pltpu.make_async_copy(w_out.at[:, pl.ds(pl.multiple_of(i * blk, blk), blk)], wo.at[i % slots], osem.at[i % slots])

    @pl.when(step < attend_at)
    def _():
        project(step, fetch[:2], gain, cos, sin, wq, wk, wv, n_out, inv_out, qb, kb, vb, ns, ws, sem, wsem)

    @pl.when(step == attend_at - 1)
    def _():
        for i in range(slots):
            load(i).start()

    @pl.when(step == attend_at)
    def _():
        wait_all(loads)
        start_all(saves[:3])

    @pl.when(step == first)
    def _():
        saves[3].start()

    @pl.when((step >= attend_at) & (step < first))
    def _():
        rows = qa.shape[0] // (2 * batch)
        attend_row(step - attend_at, rows, batch, (qa, qb), (ka, kb), (va, vb), down, across, o)

    @pl.when((step > first) & (step - first + slots - 1 < steps))
    def _():
        load(step - first + slots - 1).start()

    def share():
        load(step - first).wait()
        r = dot(o[...], wo[(step - first) % slots])
        rows = p0.shape[0]
        p0[...] = r[:rows].astype(BF16)
        p1[...] = r[rows:2 * rows].astype(BF16)
        return [(r[2 * rows:3 * rows], r[3 * rows:])]

    chip_sum(first, steps, share, [s2], *chip)

    @pl.when(step == first + steps)
    def _():
        wait_all(saves)
        fetch[2].wait()


def forward(batch, h2, gain, cos, sin, wq, wk, wv, qa, ka, va, down, across, w_out):
    half, width = h2.shape
    tok = 2 * half
    nq, nk = wq.shape[1], wk.shape[1]
    wide, blk = 2 * nk, 1024
    first, steps = nq // wide + 1 + batch, width // blk
    specs, shapes = project_out(tok, width, nq, nk)
    now = pl.BlockSpec((half, blk), lambda i: (0, clip(i - first, steps)))
    late = pl.BlockSpec((half, blk), lambda i: (0, clip(i - first - 1, steps)))
    return pl.pallas_call(
        functools.partial(forward_kernel, batch, first, steps), name="forward", grid=(first + steps + 1,),
        in_specs=[ANY] + [const_spec(x.shape) for x in (gain, cos, sin)] + [ANY] * 3
        + [ANY] * 3 + [const_spec(x.shape) for x in (down, across)] + [ANY],
        out_specs=specs[:2] + [ANY] * 5 + [now, now, late],
        out_shape=shapes + [jax.ShapeDtypeStruct((2 * tok, nq), BF16)] + [jax.ShapeDtypeStruct((half, width), BF16)] * 4,
        scratch_shapes=project_scratch(tok, width, wide) + [pltpu.VMEM((3, nq, blk), BF16), pltpu.SemaphoreType.DMA((3,))]
        + like(qa, ka, va, qa, ka, va) + [pltpu.VMEM((2 * tok, nq), BF16), pltpu.SemaphoreType.DMA((3,)), pltpu.SemaphoreType.DMA((4,)), pltpu.SemaphoreType.DMA((2, 2))]
        + chip_sum_scratch(half, blk),
        compiler_params=comm_params(0), cost_estimate=cost(2 * tok * width * (3 * nq + 2 * nk), 4 * width * nq),
    )(h2, gain, cos, sin, wq, wk, wv, qa, ka, va, down, across, w_out)


def backward_kernel(batch, heads_steps, steps, ga, gb, w_out, down, across, wq, wk, wv, h0, h1, h2, h3, inv_a, inv_b, *refs):
    kept_in, (dq_out, dk_out, dv_out, d0, d1, t2, gain), kept = refs[:11], refs[11:18], refs[18:29]
    gh_a, qa, qb, ka, kb, va, vb, ca, cb, sa, sb = kept
    grads, gs, gh_b, wo, ws, sem, osem, wsem, isem, esem = refs[29:39]
    chip = refs[39:]
    step = pl.program_id(0)
    loads = copies_of(kept_in, kept, isem)
    nq, nk = wq.shape[1], wk.shape[1]
    lanes = [pl.ds(0, nq), pl.ds(nq, nk), pl.ds(nq + nk, nk)]
    dq, dk, dv = [grads.at[:, at] for at in lanes]
    saves = copies_of((dq, dk, dv), (dq_out, dk_out, dv_out), esem)
    greet()
    half = ga.shape[0]
    slots, blk = wo.shape[:2]
    w_slots, wide = ws.shape[:2]
    first = heads_steps + batch

    def load(i):
        return pltpu.make_async_copy(w_out.at[pl.ds(pl.multiple_of(i * blk, blk), blk)], wo.at[i % slots], osem.at[i % slots])

    def load_w(i):
        at = pl.ds(pl.multiple_of(i * wide, wide), wide)
        return [pltpu.make_async_copy(w.at[at], ws.at[i % w_slots, :, lanes[j]], wsem.at[j, i % w_slots]) for j, w in enumerate((wq, wk, wv))]

    def start_w(i):
        for c in load_w(i):
            c.start()

    @pl.when(step == 0)
    def _():
        fetch = copies_of((ga, gb), (gs.at[pl.ds(0, half)], gs.at[pl.ds(half, half)]), sem)
        start_all(fetch)
        load(0).start()
        wait_all(fetch)
        for i in range(1, slots):
            load(i).start()

    @pl.when(step == heads_steps // 2)
    def _():
        start_all(loads)

    @pl.when(step == heads_steps)
    def _():
        wait_all(loads)

    @pl.when(step == first)
    def _():
        start_all(saves)

    @pl.when((step > 0) & (step + slots - 1 < heads_steps))
    def _():
        load(step + slots - 1).start()

    @pl.when(step < heads_steps)
    def _():
        load(step).wait()
        gh_b[:, pl.ds(pl.multiple_of(step * blk, blk), blk)] = dot(gs[...], wo[step % slots], NT).astype(BF16)

    @pl.when(step == heads_steps - 1)
    def _():
        for i in range(w_slots):
            start_w(i)

    @pl.when((step >= heads_steps) & (step < first))
    def _():
        rows = qa.shape[0] // (2 * batch)
        attend_back_row(step - heads_steps, rows, batch, (qa, qb), (ka, kb), (va, vb), (gh_a, gh_b), down, across, (ca, cb), (sa, sb), dq, dk, dv)

    @pl.when((step > first) & (step - first + w_slots - 1 < steps))
    def _():
        start_w(step - first + w_slots - 1)

    def share():
        i = step - first
        for c in load_w(i):
            c.wait()
        r = dot(grads[...], ws[i % w_slots], NT)
        parts = [r[j * half:(j + 1) * half] for j in range(4)]
        d0[...] = parts[0].astype(BF16)
        d1[...] = parts[1].astype(BF16)
        total = 0.0
        for j, (part, h) in enumerate(zip(parts, (h0, h1, h2, h3))):
            inv = (inv_a, inv_b)[j // 2][(j % 2) * half:(j % 2 + 1) * half, :1]
            total = total + jnp.sum(part * (h[...].astype(F32) * inv), axis=0, keepdims=True)
        total = jnp.broadcast_to(total, gain.shape)
        return [(parts[2], parts[3]), (total, total)]

    chip_sum(first, steps, share, [t2, gain], *chip)

    @pl.when(step == first + steps)
    def _():
        wait_all(saves)


def backward(batch, ga, gb, w_out, gh_a, qa, qb, ka, kb, va, vb, down, across, ca, cb, sa, sb, wq, wk, wv, h, inv_a, inv_b):
    half, width = ga.shape
    tok = 4 * half
    nq, nk = wq.shape[1], wk.shape[1]
    blk, wide = 256, 1024
    heads_steps, steps = nq // blk, width // wide
    first = heads_steps + batch
    now = pl.BlockSpec((half, wide), lambda i: (0, clip(i - first, steps)))
    late = pl.BlockSpec((half, wide), lambda i: (0, clip(i - first - 1, steps)))
    kept = (gh_a, qa, qb, ka, kb, va, vb, ca, cb, sa, sb)
    return pl.pallas_call(
        functools.partial(backward_kernel, batch, heads_steps, steps), name="backward", grid=(first + steps + 1,),
        in_specs=[ANY] * 3 + [const_spec(x.shape) for x in (down, across)] + [ANY] * 3 + [now] * 4
        + [const_spec(x.shape) for x in (inv_a, inv_b)] + [ANY] * len(kept),
        out_specs=[ANY] * 3 + [now, now, late, pl.BlockSpec((8, wide), lambda i: (0, clip(i - first - 1, steps)))],
        out_shape=[jax.ShapeDtypeStruct((tok, n), BF16) for n in (nq, nk, nk)] + [jax.ShapeDtypeStruct((half, width), BF16)] * 3
        + [jax.ShapeDtypeStruct((8, width), F32)],
        scratch_shapes=like(*kept) + [pltpu.VMEM((tok, nq + 2 * nk), BF16)]
        + [pltpu.VMEM((2 * half, width), BF16), pltpu.VMEM((2 * half, nq), BF16), pltpu.VMEM((4, blk, width), BF16),
           pltpu.VMEM((3, wide, nq + 2 * nk), BF16),
           pltpu.SemaphoreType.DMA((2,)), pltpu.SemaphoreType.DMA((4,)), pltpu.SemaphoreType.DMA((3, 3)),
           pltpu.SemaphoreType.DMA((len(kept),)), pltpu.SemaphoreType.DMA((3,))]
        + chip_sum_scratch(half + 8, wide),
        compiler_params=comm_params(1), cost_estimate=cost(2 * tok * width * (2 * nq + 2 * nk), 4 * width * nq),
    )(ga, gb, w_out, down, across, wq, wk, wv, *h, inv_a, inv_b, *kept)


def weight_grads_kernel(steps, na, nb, dq, dk, dv, o_in, g0, g1, g2, g3, p0, p1, p2, h, gq, gk, gv, g_out, out, o, ot, sem):
    step = pl.program_id(0)
    load = pltpu.make_async_copy(o_in, o, sem)

    @pl.when(step == 1)
    def _():
        load.start()

    @pl.when(step < steps)
    def _():
        n = jnp.concatenate([na[...], nb[...]], axis=0).T
        for d, grad in ((dq, gq), (dk, gk), (dv, gv)):
            grad[...] = dot(n, d[...])

    @pl.when(step == steps)
    def _():
        load.wait()
        for c in range(0, o.shape[1], 256):
            ot[c:c + 256, :] = o[:, c:c + 256].T

    @pl.when(step >= steps)
    def _():
        g_out[...] = dot(ot[...], jnp.concatenate([g0[...], g1[...], g2[...], g3[...]], axis=0))
        share = sum(x[...].astype(F32) for x in (p0, p1, p2))
        out[...] = (h[...].astype(F32) + share.astype(BF16).astype(F32)).astype(BF16)


def weight_grads(na, nb, dq, dk, dv, o, g, p, h):
    tok, nq = dq.shape
    nk = dk.shape[1]
    width = na.shape[1]
    blk = 1024
    steps = width // blk

    def early(i):
        return jnp.minimum(i, steps - 1)

    def late(i):
        return jnp.maximum(i - steps, 0)

    rows = pl.BlockSpec((tok // 4, blk), lambda i: (0, late(i)))
    return pl.pallas_call(
        functools.partial(weight_grads_kernel, steps), name="weight_grads", grid=(2 * steps,),
        in_specs=[pl.BlockSpec((tok // 2, blk), lambda i: (0, early(i)))] * 2 + [const_spec((tok, nq))] + [const_spec((tok, nk))] * 2
        + [ANY] + [rows] * 8,
        out_specs=[pl.BlockSpec((blk, n), lambda i: (early(i), 0)) for n in (nq, nk, nk)] + [pl.BlockSpec((nq, blk), lambda i: (0, late(i))), rows],
        out_shape=[jax.ShapeDtypeStruct((width, n), F32) for n in (nq, nk, nk)]
        + [jax.ShapeDtypeStruct((nq, width), F32), jax.ShapeDtypeStruct(h.shape, BF16)],
        scratch_shapes=[pltpu.VMEM((tok, nq), BF16), pltpu.VMEM((nq, tok), BF16), pltpu.SemaphoreType.DMA],
        compiler_params=params(56), cost_estimate=cost(4 * tok * width * (nq + nk), 8 * width * (nq + nk)),
    )(na, nb, dq, dk, dv, o, *g, *p, h)


def norm_back_kernel(d0, d1, d2, h, g, inv, gain, gg0, gg1, grad, grad_gain, *refs):
    held, out, dg, isem, esem = refs
    rows, width = dg.shape
    count = out.shape[0] // rows
    wide = 512

    def at(i):
        return pl.ds(pl.multiple_of(i * rows, rows), rows)

    def load(i):
        return pltpu.make_async_copy(d2.at[at(i)], held.at[at(i)], isem.at[i])

    def save(i):
        return pltpu.make_async_copy(out.at[at(i)], grad.at[at(i)], esem.at[i])

    @pl.loop(0, count)
    def _(i):
        load(i).start()

    grad_gain[...] = gg0[0:1] + gg1[0:1]
    x0, x1, x2, hs, gs = d0, d1, held, h, g

    @pl.loop(0, count)
    def _(i):
        load(i).wait()
        total = jnp.zeros((rows, wide), F32)
        for c in range(0, width, wide):
            cut = slice(c, c + wide)
            x = sum(d[at(i), cut].astype(F32) for d in (x0, x1, x2)) * gain[:, cut]
            dg[:, cut] = x
            total = total + x * hs[at(i), cut].astype(F32)
        s = inv[at(i), :1]
        back = (s * s * s) * (jnp.sum(total, axis=-1, keepdims=True) / width)
        s = jnp.broadcast_to(s, (rows, wide))
        back = jnp.broadcast_to(back, (rows, wide))
        for c in range(0, width, wide):
            cut = slice(c, c + wide)
            out[at(i), cut] = (gs[at(i), cut].astype(F32) + (s * dg[:, cut] - hs[at(i), cut].astype(F32) * back)).astype(BF16)
        save(i).start()

    @pl.loop(0, count)
    def _(i):
        save(i).wait()


def norm_back(d, h, g, inv, gain, gain_shares):
    tok, width = h.shape
    rows = 48
    count = tok // rows
    whole = pl.BlockSpec(memory_space=pltpu.VMEM)
    return pl.pallas_call(
        norm_back_kernel, name="norm_back", in_specs=[whole] * 2 + [ANY] + [whole] * 6, out_specs=[ANY, whole],
        out_shape=[jax.ShapeDtypeStruct((tok, width), BF16), jax.ShapeDtypeStruct((1, width), F32)],
        scratch_shapes=[pltpu.VMEM((tok, width), BF16)] * 2
        + [pltpu.VMEM((rows, width), F32), pltpu.SemaphoreType.DMA((count,)), pltpu.SemaphoreType.DMA((count,))],
        compiler_params=pltpu.CompilerParams(vmem_limit_bytes=20 << 20), cost_estimate=cost(20 * tok * width, 12 * tok * width),
    )(*d, h, g, inv, gain, *gain_shares)


def solution(mesh):
    tp_size = mesh.shape['tp']
    beside = [(i, i ^ 1) for i in range(tp_size)]
    across = [(i, i ^ 2) for i in range(tp_size)]

    def send(x, pairs):
        return lax.ppermute(x, 'tp', pairs)

    def after(x, *others):
        return lax.optimization_barrier((x,) + others)[0]

    def step(hidden, positions, doc_ids, norm_gain, w_query, w_key, w_value, w_out, grad_out):
        batch, rows, width = hidden.shape
        tok = batch * rows
        nq, nk = w_query.shape[1], w_key.shape[1]
        group = nq // nk
        gain = norm_gain.astype(F32).reshape(1, width)

        pos1, doc1 = send(positions, beside), send(doc_ids, beside)
        pos2, doc2 = send(positions, across), send(doc_ids, across)
        h0 = hidden.reshape(tok, width)
        g0 = grad_out.reshape(tok, width)
        h2 = send(h0, across)
        h1 = send(h0, beside)
        g1 = send(g0, beside)
        g2 = send(g0, across)

        lane = jnp.arange(HEAD_DIM)
        inv_freq = ROPE_BASE ** (-(lane // 2 * 2).astype(F32) / HEAD_DIM)
        sign = jnp.where(lane % 2 == 0, -1.0, 1.0)

        def tables(*pos):
            angles = jnp.stack(pos).astype(F32)[..., None] * inv_freq
            return jnp.cos(angles), jnp.sin(angles) * sign

        ca, sa = [x.reshape(2 * tok, HEAD_DIM) for x in tables(positions, pos1)]
        na, inv_a, qa, ka, va = qkv(h0, h1, gain, ca, sa, w_query, w_key, w_value)
        pos2, doc2, ka = lax.optimization_barrier((pos2, doc2, ka))
        pos3, doc3 = send(pos2, beside), send(doc2, beside)
        cb, sb = [x.reshape(2 * tok, HEAD_DIM) for x in tables(pos2, pos3)]
        both = jnp.stack([jnp.concatenate([doc_ids, doc1, doc2, doc3], axis=1), jnp.concatenate([positions, pos1, pos2, pos3], axis=1)], axis=1)
        down, over = jnp.swapaxes(both, 1, 2), jnp.tile(both, (1, 1, group))
        dha = heads_grad(g0, g1, w_out, ka, cb, sb, down, over)
        nb, inv_b, qb, kb, vb, o, h3, p0, p1, s2 = forward(
            batch, h2, gain, cb, sb, w_query, w_key, w_value, qa, ka, va, down, over, w_out)
        s2 = send(s2, across)
        g3 = send(after(g2, p0), beside)
        p1 = send(p1, beside)
        dq, dk, dv, d0, d1, t2, gg = backward(
            batch, g2, g3, w_out, dha, qa, qb, ka, kb, va, vb, down, over, ca, cb, sa, sb,
            w_query, w_key, w_value, (h0, h1, h2, h3), inv_a, inv_b)
        t2, d1, gg, dq = lax.optimization_barrier((t2, d1, gg, dq))
        t2 = send(t2, across)
        d1 = send(d1, beside)
        gg2 = send(gg, across)
        gq, gk, gv, g_out, attn_out = weight_grads(na, nb, dq, dk, dv, o, (g0, g1, g2, g3), (p0, p1, s2), h0)
        grad_hidden, gg = norm_back((after(d0, gk), d1, t2), h0, g0, inv_a[:tok], gain, (gg, gg2))
        grad_gain = gg.reshape(width)
        attn_out, grad_hidden = attn_out.reshape(hidden.shape), grad_hidden.reshape(hidden.shape)
        return (attn_out, grad_hidden, grad_gain, gq, gk, gv, g_out)

    row_spec = P('dp', 'tp', None)
    tok_spec = P('dp', 'tp')
    col_spec = P(None, 'tp')

    return jax.shard_map(
        step, mesh=mesh,
        in_specs=(row_spec, tok_spec, tok_spec, P(), col_spec, col_spec, col_spec, P('tp', None), row_spec),
        out_specs=(row_spec, row_spec, P('dp'), P('dp', 'tp'), P('dp', 'tp'), P('dp', 'tp'), P(('dp', 'tp'), None)),
        check_vma=False)
```
